32 devices in a mesh: row: 4 (over x, core), col: 8 (over z, y).
Axes of the slice: x: 2, y: 2, z: 4, core: 2. Of those that a mesh axis runs over, the one named last changes fastest.
Arguments:
- moment_x: float32 [496, 496], P('row', 'col'), may hold values from -8 to 8
- zinv: float32 [496, 496], P('row', 'col'), may hold values from -8 to 8
- positions: int32 [1024, 16], P(('row', 'col')), may hold values from 0 to 495
- entry_count: int32 [1024], P(('row', 'col')), may hold values from 1 to 8
Outputs:
- schur: float32 [1024, 1024], P('row', 'col')
The draws below stay inside these ranges and needn't reach their ends.
All inputs are finite; a program needn't handle non-finite values.
Results may differ from the reference program's by a relative error of at most 0.0003.
Values sent between devices are 32-bit elements; how exact they have to be, the bound alone decides.
No kernel may reach another device: no remote copies, remote signals or barrier semaphores. Data moves between devices by JAX's collectives and lax.ppermute only.
A program may use at most 64 MiB of HBM per device.

```python
import jax
import jax.numpy as jnp
from jax import lax

NMON = 496
SLOTS = 8
CONS = 1024


def symmetric_draw(key):
    key_a = jax.random.fold_in(key, 11)
    key_s = jax.random.fold_in(key, 23)
    base = jax.random.normal(key_a, (NMON, NMON), jnp.float32)
    scales = jnp.exp(jax.random.uniform(key_s, (NMON,), jnp.float32, -0.5, 0.47))
    mixed = 0.5 * (base + base.T) * scales[:, None] * scales[None, :]
    return jnp.clip(mixed, -8.0, 8.0)


def draw_moment_x(key, part):
    return symmetric_draw(jax.random.fold_in(key, 101))


def draw_zinv(key, part):
    return symmetric_draw(jax.random.fold_in(key, 202))


def set_ends(array, own_key, low, top_value):
    spot = [jax.random.randint(jax.random.fold_in(own_key, axis), (), 0, length) for axis, length in enumerate(array.shape)]
    main_axis = array.shape.index(max(array.shape))
    next_to = spot[:main_axis] + [(spot[main_axis] + 1) % array.shape[main_axis]] + spot[main_axis + 1:]
    return array.at[tuple(spot)].set(low).at[tuple(next_to)].set(top_value)


def setup_inputs(seed: int = 0) -> dict:
    key_list = jax.random.split(jax.random.key(seed), 5)
    moment_x = draw_moment_x(jax.random.fold_in(key_list[4], 71), 0)
    zinv = draw_zinv(jax.random.fold_in(key_list[4], 71), 0)
    positions = set_ends(jax.random.randint(key_list[2], (CONS, 2 * SLOTS), 0, NMON), jax.random.fold_in(key_list[2], 1), 0, NMON - 1).astype(jnp.int32)
    entry_count = set_ends(jax.random.randint(key_list[3], (CONS,), 1, SLOTS + 1), jax.random.fold_in(key_list[3], 1), 1, SLOTS).astype(jnp.int32)
    return dict(moment_x=moment_x, zinv=zinv, positions=positions, entry_count=entry_count)


def schur_rows(moment_x, zinv, row_positions, row_counts, col_positions, col_counts, group_rows):
    slot_count = row_positions.shape[1] // 2
    slot_iota = jnp.arange(slot_count, dtype=jnp.int32)
    col_left = col_positions[:, :slot_count].reshape(-1)
    col_right = col_positions[:, slot_count:].reshape(-1)
    col_alive = (slot_iota[None, :] < col_counts[:, None]).astype(jnp.float32).reshape(-1)
    ncols = col_positions.shape[0]
    nrows = row_positions.shape[0]

    def one_group(packed):
        grp_positions, grp_counts = packed
        grp_left = grp_positions[:, :slot_count].reshape(-1)
        grp_right = grp_positions[:, slot_count:].reshape(-1)
        grp_alive = (slot_iota[None, :] < grp_counts[:, None]).astype(jnp.float32).reshape(-1)
        x_picked = jnp.take(jnp.take(moment_x, grp_right, axis=0), col_left, axis=1)
        w_picked = jnp.take(jnp.take(zinv, col_right, axis=0), grp_left, axis=1)
        terms = x_picked * w_picked.T * grp_alive[:, None] * col_alive[None, :]
        return jnp.sum(terms.reshape(group_rows, slot_count, ncols, slot_count), axis=(1, 3))

    grouped = (row_positions.reshape(nrows // group_rows, group_rows, 2 * slot_count),
               row_counts.reshape(nrows // group_rows, group_rows))
    return lax.map(one_group, grouped).reshape(nrows, ncols)


def reference(moment_x, zinv, positions, entry_count):
    return schur_rows(moment_x, zinv, positions, entry_count, positions, entry_count, 64)
```

```python
import functools
import jax
import jax.numpy as jnp
from jax import lax
from jax.experimental import pallas as pl
from jax.experimental.pallas import tpu as pltpu
from jax.sharding import PartitionSpec as P

LANES = 128
F32, BF16, I32 = jnp.float32, jnp.bfloat16, jnp.int32


class Plan:
    def __init__(self, rows, cols, x_shape, pos_shape):
        self.rows, self.cols = rows, cols
        self.mb, self.nb = x_shape
        self.order = self.mb * rows
        self.halves = self.mb // self.nb
        self.slot = 1 << self.nb.bit_length()
        self.depth = cols * self.slot
        self.dead = self.slot - 1
        self.local, self.slots = pos_shape[0], pos_shape[1] // 2
        self.per_tile = LANES // self.local
        self.ni = self.local * cols
        self.nj = self.local * rows
        self.x_at, self.z_at, self.p_at = 0, self.slot, 2 * self.slot
        self.payload = 2 * self.slot + 2 * self.slots
        row_bits = [b for b in range(rows.bit_length() - 1)]
        col_bits = [b for b in range(cols.bit_length() - 1)]
        self.steps = [("row", b) for b in row_bits[1:]]
        self.steps += [("col", b) for b in col_bits]
        self.steps += [("row", 0)]

    def place(self, row_xor, col_xor):
        out = 0
        for n, (axis, bit) in enumerate(self.steps):
            value = row_xor if axis == "row" else col_xor
            out = out | (((value >> bit) & 1) << n)
        return out


def pack_kernel(plan, x_ref, z_ref, pos_ref, cnt_ref, out_ref):
    nb, slot = plan.nb, plan.slot
    out_ref[...] = jnp.zeros_like(out_ref)
    zt = z_ref[...].T
    for h in range(plan.halves):
        out_ref[0:nb, h * slot : h * slot + nb] = x_ref[h * nb : (h + 1) * nb, :]
        out_ref[slot : slot + nb, h * slot : h * slot + nb] = zt[:, h * nb : (h + 1) * nb]
    spots = pos_ref[...].astype(F32).T
    code = spots
    for t in range(1, plan.cols):
        code = code + jnp.where(spots >= float(t * nb), float(slot - nb), 0.0)
    k = lax.broadcasted_iota(I32, code.shape, 0) % plan.slots
    code = jnp.where(k < cnt_ref[...], code, float(plan.dead))
    wide = jnp.concatenate([code] * plan.per_tile, axis=1)
    me = lax.axis_index("row") * plan.cols + lax.axis_index("col")
    mine = lax.broadcasted_iota(I32, wide.shape, 1) // plan.local == me % plan.per_tile
    out_ref[plan.p_at :, :] = jnp.where(mine, wide, 0.0)


def main_kernel(plan, g_ref, out_ref, xj, zj, pick, ivec, acc, idx, sem):
    slot, halves, cols, rows = plan.slot, plan.halves, plan.cols, plan.rows
    slots, tiles = plan.slots, plan.ni // LANES
    me_r, me_c = lax.axis_index("row"), lax.axis_index("col")
    chunk = pl.program_id(0)
    group_of = me_c // plan.per_tile

    def codes(row, group):
        at = row ^ me_r
        total = None
        for e in range(plan.per_tile):
            cx = (group ^ group_of) * plan.per_tile + e
            part = g_ref[plan.place(at, cx), plan.p_at :, :]
            total = part if total is None else total + part
        return total.astype(I32)

    for t in range(tiles):
        ivec[t] = codes(me_r, t)
    copy = pltpu.make_async_copy(ivec, idx, sem)
    copy.start()

    tile_at = me_c * (plan.nj // LANES) + chunk
    jcode = codes(tile_at // (cols // plan.per_tile), tile_at % (cols // plan.per_tile))
    depth_iota = lax.broadcasted_iota(I32, (plan.depth, LANES), 0)
    lane = lax.broadcasted_iota(I32, (slot, LANES), 1)
    per_group = LANES // slot

    def block(row, col, at):
        return g_ref[plan.place(row ^ me_r, col ^ me_c), at : at + slot, :]

    def split(v):
        hi = v.astype(BF16)
        lo = (v - hi.astype(F32)).astype(BF16)
        return hi, lo

    def select(left, out):
        hi, lo = split(left)
        both = jnp.concatenate([hi, lo], axis=0)
        res = jnp.dot(both, pick[...], preferred_element_type=F32)
        res = res[:slot] + res[slot:]
        for l in range(slots):
            out[pl.ds(l, slot, stride=slots), :] = res[:, l * LANES : (l + 1) * LANES]

    for l in range(slots):
        at = jcode[l : l + 1, :]
        pick[:, l * LANES : (l + 1) * LANES] = jnp.where(depth_iota == at, 1.0, 0.0).astype(BF16)
    for r in range(rows):
        for h in range(halves):
            parts = []
            for g in range(cols // per_group):
                part = None
                for e in range(per_group):
                    v = block(r, g * per_group + e, plan.x_at)
                    if e != h:
                        v = pltpu.roll(v, ((e - h) * slot) % LANES, 1)
                    part = v if part is None else jnp.where(lane // slot == e, v, part)
                parts.append(part)
            u = r * halves + h
            select(jnp.concatenate(parts, axis=1), xj.at[pl.ds(u * slot * slots, slot * slots), :])
    for l in range(slots):
        at = jcode[slots + l : slots + l + 1, :]
        pick[:, l * LANES : (l + 1) * LANES] = jnp.where(depth_iota == at, 1.0, 0.0).astype(BF16)
    wide = halves * slot
    for c in range(cols):
        parts = []
        for g in range(rows * wide // LANES):
            part = None
            for e in range(LANES // wide):
                v = block(g * (LANES // wide) + e, c, plan.z_at)
                if e:
                    v = pltpu.roll(v, e * wide, 1)
                part = v if part is None else jnp.where(lane // wide == e, v, part)
            parts.append(part)
        select(jnp.concatenate(parts, axis=1), zj.at[pl.ds(c * slot * slots, slot * slots), :])

    copy.wait()

    def eight(n, _):
        tile, base = n // (LANES // 8), (n % (LANES // 8)) * 8
        for s in range(8):
            total = None
            for k in range(slots):
                q = pl.multiple_of(idx[tile, slots + k, base + s] * slots, slots)
                p = pl.multiple_of(idx[tile, k, base + s] * slots, slots)
                term = xj[pl.ds(q, slots), :] * zj[pl.ds(p, slots), :]
                total = term if total is None else total + term
            acc[s * slots : (s + 1) * slots, :] = total
        out = None
        for l in range(slots):
            v = acc[pl.ds(l, 8, stride=slots), :]
            out = v if out is None else out + v
        out_ref[pl.ds(pl.multiple_of(n * 8, 8), 8), :] = out
        return 0

    lax.fori_loop(0, plan.ni // 8, eight, 0)


def gather(plan, v):
    for axis, bit in plan.steps:
        size = plan.rows if axis == "row" else plan.cols
        other = lax.ppermute(v, axis, [(d, d ^ (1 << bit)) for d in range(size)])
        v = jnp.concatenate([v, other], axis=0)
    return v


def shards(rows, cols, moment_x, zinv, positions, entry_count):
    plan = Plan(rows, cols, moment_x.shape, positions.shape)
    packed = pl.pallas_call(
        functools.partial(pack_kernel, plan),
        out_shape=jax.ShapeDtypeStruct((plan.payload, LANES), F32),
        name="pack",
    )(moment_x, zinv, positions, entry_count.reshape(1, -1))
    whole = gather(plan, packed[None])
    return pl.pallas_call(
        functools.partial(main_kernel, plan),
        grid=(plan.nj // LANES,),
        in_specs=[pl.BlockSpec(memory_space=pltpu.VMEM)],
        out_specs=pl.BlockSpec((plan.ni, LANES), lambda c: (0, c)),
        out_shape=jax.ShapeDtypeStruct((plan.ni, plan.nj), F32),
        scratch_shapes=[
            pltpu.VMEM((plan.depth * plan.slots, LANES), F32),
            pltpu.VMEM((plan.depth * plan.slots, LANES), F32),
            pltpu.VMEM((plan.depth, plan.slots * LANES), BF16),
            pltpu.VMEM((plan.ni // LANES, 2 * plan.slots, LANES), I32),
            pltpu.VMEM((8 * plan.slots, LANES), F32),
            pltpu.SMEM((plan.ni // LANES, 2 * plan.slots, LANES), I32),
            pltpu.SemaphoreType.DMA,
        ],
        name="schur",
    )(whole)


def solution(mesh):
    return jax.shard_map(
        functools.partial(shards, mesh.shape["row"], mesh.shape["col"]),
        mesh=mesh,
        in_specs=(P("row", "col"), P("row", "col"), P(("row", "col"), None), P(("row", "col"))),
        out_specs=P("row", "col"),
        check_vma=False,
    )
```

```python
import functools
import itertools
import jax
import jax.numpy as jnp
from jax import lax
from jax.experimental import pallas as pl
from jax.experimental.pallas import tpu as pltpu
from jax.sharding import PartitionSpec as P

LANES = 128
F32, BF16, I32 = jnp.float32, jnp.bfloat16, jnp.int32
EXTRA = 8


class Plan:
    def __init__(self, rows, cols, x_shape, pos_shape):
        self.rows, self.cols = rows, cols
        self.mb, self.nb = x_shape
        self.halves = self.mb // self.nb
        self.slot = 1 << self.nb.bit_length()
        self.wide = self.halves * self.slot
        self.depth = cols * self.slot
        self.dead = self.slot - 1
        self.local, self.slots = pos_shape[0], pos_shape[1] // 2
        self.fold = LANES // self.local
        self.folded = 2 * self.slots // self.fold
        self.ni = self.local * cols
        self.nj = self.local * rows
        self.payload = self.slot + EXTRA
        row_bits, col_bits = rows.bit_length() - 1, cols.bit_length() - 1
        y_bits = col_bits // 2
        self.far = [(0, k << y_bits) for k in range(1 << (col_bits - y_bits))]
        self.near = [(i << 1, k) for i in range(1 << (row_bits - 1)) for k in range(1 << y_bits)]


def pack_kernel(plan, x_ref, z_ref, pos_ref, cnt_ref, out_ref):
    nb, slot, wide = plan.nb, plan.slot, plan.wide
    me_r, me_c = lax.axis_index("row"), lax.axis_index("col")
    out_ref[...] = jnp.zeros_like(out_ref)
    a = lax.broadcasted_iota(I32, (nb, plan.mb), 0) + me_c * nb
    b = lax.broadcasted_iota(I32, (nb, plan.mb), 1) + me_r * plan.mb
    z = z_ref[...]
    mixed = jnp.where(a <= b, x_ref[...], z)
    diag = jnp.sum(jnp.where(a == b, z, 0.0), axis=0, keepdims=True)
    at = slot + plan.folded
    for h in range(plan.halves):
        out_ref[0:nb, h * slot : h * slot + nb] = mixed[:, h * nb : (h + 1) * nb]
        out_ref[at : at + 1, h * slot : h * slot + nb] = diag[:, h * nb : (h + 1) * nb]
    spots = pos_ref[...].astype(F32)
    code = spots
    for t in range(1, plan.cols):
        code = code + jnp.where(spots >= float(t * nb), float(slot - nb), 0.0)
    k = lax.broadcasted_iota(I32, code.shape, 0) % plan.slots
    code = jnp.where(k < cnt_ref[...], code, float(plan.dead))
    for g in range(plan.fold):
        piece = code[g * plan.folded : (g + 1) * plan.folded, :]
        out_ref[slot : slot + plan.folded, g * plan.local : (g + 1) * plan.local] = piece


def main_kernel(plan, n_in, *refs):
    ins, out_ref = refs[:n_in], refs[n_in]
    misc, mat, left, xj, zj, pick, ivec, acc, idx, sem = refs[n_in + 1 :]
    slot, cols, rows = plan.slot, plan.cols, plan.rows
    slots, tiles, depth = plan.slots, plan.ni // LANES, plan.depth
    me_r, me_c = lax.axis_index("row"), lax.axis_index("col")
    chunk = pl.program_id(0)
    per = LANES // plan.wide
    if per > 1:
        mat[...] = jnp.zeros_like(mat)
    near = [(core ^ i, k) for core in (0, 1) for i, k in plan.near]
    for ref, (ri, ci) in zip(ins, near):
        for n, (rf, cf) in enumerate(plan.far):
            r, c = me_r ^ (ri ^ rf), me_c ^ (ci ^ cf)
            misc[r * cols + c] = ref[n, slot:, :]
            v = ref[n, 0:slot, :]
            span = pl.ds(pl.multiple_of(c * slot, slot), slot)
            if per == 1:
                mat[r, span, :] = v
            else:
                mat[r // per, span, :] += pltpu.roll(v, (r % per) * plan.wide, 1)

    lane = lax.broadcasted_iota(I32, (plan.folded, LANES), 1) // plan.local

    def codes(first):
        got = [misc[first + e][0 : plan.folded] for e in range(plan.fold)]
        quads = []
        for g in range(plan.fold):
            quad = None
            for e in range(plan.fold):
                v = got[e]
                if e != g:
                    v = pltpu.roll(v, ((e - g) * plan.local) % LANES, 1)
                quad = v if quad is None else jnp.where(lane == e, v, quad)
            quads.append(quad)
        return jnp.concatenate(quads, axis=0).astype(I32)

    for t in range(tiles):
        ivec[t] = codes(me_r * cols + t * plan.fold) * slots
    copy = pltpu.make_async_copy(ivec, idx, sem)
    copy.start()
    jcode = codes(me_c * rows + chunk * plan.fold)

    depth_iota = lax.broadcasted_iota(I32, (depth, LANES), 0)
    n_tile = depth // LANES
    ra = lax.broadcasted_iota(I32, (LANES, LANES), 0)
    rb = lax.broadcasted_iota(I32, (LANES, LANES), 1)

    def tile(i, j):
        return mat[j, i * LANES : (i + 1) * LANES, :]

    def put(i, j, v):
        hi = v.astype(BF16)
        lo = (v - hi.astype(F32)).astype(BF16)
        left[i * LANES : (i + 1) * LANES, j * LANES : (j + 1) * LANES] = hi
        left[depth + i * LANES : depth + (i + 1) * LANES, j * LANES : (j + 1) * LANES] = lo

    def select(base, out):
        for l in range(slots):
            at = jcode[base + l : base + l + 1, :]
            pick[:, l * LANES : (l + 1) * LANES] = jnp.where(depth_iota == at, 1.0, 0.0).astype(BF16)
        for m in range(slots // 2):
            res = jnp.dot(left[...], pick[:, m * 256 : (m + 1) * 256], preferred_element_type=F32)
            res = res[:depth] + res[depth:]
            for l in range(2):
                out[pl.ds(2 * m + l, depth, stride=slots), :] = res[:, l * LANES : (l + 1) * LANES]

    for i in range(n_tile):
        for j in range(i, n_tile):
            v = tile(i, j)
            if i == j:
                put(i, i, jnp.where(ra <= rb, v, v.T))
            else:
                put(i, j, v)
                put(j, i, v.T)
    select(0, xj)
    per_tile = LANES // slot
    for i in range(n_tile):
        for j in range(i, n_tile):
            v = tile(j, i)
            if i == j:
                diag = None
                for c in range(i * per_tile, (i + 1) * per_tile):
                    r = c // plan.halves
                    row = misc[r * cols + c][plan.folded : plan.folded + 1]
                    if per > 1 and r % per:
                        row = pltpu.roll(row, (r % per) * plan.wide, 1)
                    diag = row if diag is None else diag + row
                put(i, i, jnp.where(ra > rb, v, jnp.where(ra == rb, diag, v.T)))
            else:
                put(j, i, v)
                put(i, j, v.T)
    select(slots, zj)
    copy.wait()

    def eight(n, _):
        tile_at, base = n // (LANES // 8), (n % (LANES // 8)) * 8
        for s in range(8):
            total = None
            for k in range(slots):
                q = pl.multiple_of(idx[tile_at, slots + k, base + s], slots)
                p = pl.multiple_of(idx[tile_at, k, base + s], slots)
                term = xj[pl.ds(q, slots), :] * zj[pl.ds(p, slots), :]
                total = term if total is None else total + term
            acc[s * slots : (s + 1) * slots, :] = total
        out = None
        for l in range(slots):
            v = acc[pl.ds(l, 8, stride=slots), :]
            out = v if out is None else out + v
        out_ref[pl.ds(pl.multiple_of(n * 8, 8), 8), :] = out
        return 0

    lax.fori_loop(0, plan.ni // 8, eight, 0)


def send(plan, v, row_xor, col_xor):
    size = plan.cols
    pairs = []
    for r, c in itertools.product(range(plan.rows), range(plan.cols)):
        pairs.append((r * size + c, (r ^ row_xor) * size + (c ^ col_xor)))
    return lax.ppermute(v, ("row", "col"), pairs)


def gather(plan, v):
    line = [v if k == (0, 0) else send(plan, v, *k) for k in plan.far]
    stack = jnp.stack(line)
    stacks = [stack if k == (0, 0) else send(plan, stack, *k) for k in plan.near]
    return stacks + [send(plan, s, 1, 0) for s in stacks]


def schur_call(plan, stacks):
    n_tile = plan.depth // LANES
    return pl.pallas_call(
        functools.partial(main_kernel, plan, len(stacks)),
        grid=(plan.nj // LANES,),
        in_specs=[pl.BlockSpec(memory_space=pltpu.VMEM)] * len(stacks),
        out_specs=pl.BlockSpec((plan.ni, LANES), lambda c: (0, c)),
        out_shape=jax.ShapeDtypeStruct((plan.ni, plan.nj), F32),
        scratch_shapes=[
            pltpu.VMEM((plan.rows * plan.cols, EXTRA, LANES), F32),
            pltpu.VMEM((n_tile, plan.depth, LANES), F32),
            pltpu.VMEM((2 * plan.depth, plan.depth), BF16),
            pltpu.VMEM((plan.depth * plan.slots, LANES), F32),
            pltpu.VMEM((plan.depth * plan.slots, LANES), F32),
            pltpu.VMEM((plan.depth, plan.slots * LANES), BF16),
            pltpu.VMEM((plan.ni // LANES, 2 * plan.slots, LANES), I32),
            pltpu.VMEM((8 * plan.slots, LANES), F32),
            pltpu.SMEM((plan.ni // LANES, 2 * plan.slots, LANES), I32),
            pltpu.SemaphoreType.DMA,
        ],
        compiler_params=pltpu.CompilerParams(vmem_limit_bytes=24 << 20),
        name="schur",
    )(*stacks)


def shards(rows, cols, moment_x, zinv, positions, entry_count):
    plan = Plan(rows, cols, moment_x.shape, positions.shape)
    packed = pl.pallas_call(
        functools.partial(pack_kernel, plan),
        out_shape=jax.ShapeDtypeStruct((plan.payload, LANES), F32),
        compiler_params=pltpu.CompilerParams(vmem_limit_bytes=4 << 20),
        name="pack",
    )(moment_x.T, zinv.T, positions.T, entry_count.reshape(1, -1))
    return schur_call(plan, gather(plan, packed))


def solution(mesh):
    return jax.shard_map(
        functools.partial(shards, mesh.shape["row"], mesh.shape["col"]),
        mesh=mesh,
        in_specs=(P("row", "col"), P("row", "col"), P(("row", "col"), None), P(("row", "col"))),
        out_specs=P("row", "col"),
        check_vma=False,
    )
```

```python
import functools
import itertools
import jax
import jax.numpy as jnp
from jax import lax
from jax.experimental import pallas as pl
from jax.experimental.pallas import tpu as pltpu
from jax.sharding import PartitionSpec as P

LANES = 128
F32, BF16, I32 = jnp.float32, jnp.bfloat16, jnp.int32
EXTRA = 8


class Plan:
    def __init__(self, rows, cols, x_shape, pos_shape):
        self.rows, self.cols = rows, cols
        self.mb, self.nb = x_shape
        self.halves = self.mb // self.nb
        self.slot = 1 << self.nb.bit_length()
        self.wide = self.halves * self.slot
        self.depth = cols * self.slot
        self.dead = self.slot - 1
        self.local, self.slots = pos_shape[0], pos_shape[1] // 2
        self.fold = LANES // self.local
        self.folded = 2 * self.slots // self.fold
        self.ni = self.local * cols
        self.nj = self.local * rows
        self.payload = self.slot + EXTRA
        row_bits, col_bits = rows.bit_length() - 1, cols.bit_length() - 1
        y_bits = col_bits // 2
        self.far = [(0, k << y_bits) for k in range(1 << (col_bits - y_bits))]
        self.near = [(i << 1, k) for i in range(1 << (row_bits - 1)) for k in range(1 << y_bits)]


def pack_kernel(plan, x_ref, z_ref, pos_ref, cnt_ref, out_ref):
    nb, slot, wide = plan.nb, plan.slot, plan.wide
    me_r, me_c = lax.axis_index("row"), lax.axis_index("col")
    out_ref[...] = jnp.zeros_like(out_ref)
    a = lax.broadcasted_iota(I32, (nb, plan.mb), 0) + me_c * nb
    b = lax.broadcasted_iota(I32, (nb, plan.mb), 1) + me_r * plan.mb
    z = z_ref[...]
    mixed = jnp.where(a <= b, x_ref[...], z)
    diag = jnp.sum(jnp.where(a == b, z, 0.0), axis=0, keepdims=True)
    at = slot + plan.folded
    for h in range(plan.halves):
        out_ref[0:nb, h * slot : h * slot + nb] = mixed[:, h * nb : (h + 1) * nb]
        out_ref[at : at + 1, h * slot : h * slot + nb] = diag[:, h * nb : (h + 1) * nb]
    spots = pos_ref[...].astype(F32)
    code = spots
    for t in range(1, plan.cols):
        code = code + jnp.where(spots >= float(t * nb), float(slot - nb), 0.0)
    k = lax.broadcasted_iota(I32, code.shape, 0) % plan.slots
    code = jnp.where(k < cnt_ref[...], code, float(plan.dead))
    for g in range(plan.fold):
        piece = code[g * plan.folded : (g + 1) * plan.folded, :]
        out_ref[slot : slot + plan.folded, g * plan.local : (g + 1) * plan.local] = piece


def main_kernel(plan, n_in, *refs):
    ins, out_ref = refs[:n_in], refs[n_in]
    misc, mat, left, xj, zj, pick, ivec, acc, idx, sem = refs[n_in + 1 :]
    slot, cols, rows = plan.slot, plan.cols, plan.rows
    slots, tiles, depth = plan.slots, plan.ni // LANES, plan.depth
    me_r, me_c = lax.axis_index("row"), lax.axis_index("col")
    chunk = pl.program_id(0)
    per = LANES // plan.wide
    if per > 1:
        mat[...] = jnp.zeros_like(mat)
    near = [(core ^ i, k) for core in (0, 1) for i, k in plan.near]
    for ref, (ri, ci) in zip(ins, near):
        for n, (rf, cf) in enumerate(plan.far):
            r, c = me_r ^ (ri ^ rf), me_c ^ (ci ^ cf)
            misc[r * cols + c] = ref[n, slot:, :]
            v = ref[n, 0:slot, :]
            span = pl.ds(pl.multiple_of(c * slot, slot), slot)
            if per == 1:
                mat[r, span, :] = v
            else:
                mat[r // per, span, :] += pltpu.roll(v, (r % per) * plan.wide, 1)

    lane = lax.broadcasted_iota(I32, (plan.folded, LANES), 1) // plan.local

    def codes(first):
        got = [misc[first + e][0 : plan.folded] for e in range(plan.fold)]
        quads = []
        for g in range(plan.fold):
            quad = None
            for e in range(plan.fold):
                v = got[e]
                if e != g:
                    v = pltpu.roll(v, ((e - g) * plan.local) % LANES, 1)
                quad = v if quad is None else jnp.where(lane == e, v, quad)
            quads.append(quad)
        return jnp.concatenate(quads, axis=0).astype(I32)

    for t in range(tiles):
        ivec[t] = codes(me_r * cols + t * plan.fold) * slots
    copies = []
    for n in range(tiles * 2 * slots):
        spot = idx.at[pl.ds(n * LANES, LANES)]
        copies.append(pltpu.make_async_copy(ivec.at[n // (2 * slots), n % (2 * slots)], spot, sem.at[n]))
        copies[-1].start()
    jcode = codes(me_c * rows + chunk * plan.fold)

    depth_iota = lax.broadcasted_iota(I32, (depth, LANES), 0)
    n_tile = depth // LANES
    ra = lax.broadcasted_iota(I32, (LANES, LANES), 0)
    rb = lax.broadcasted_iota(I32, (LANES, LANES), 1)

    def tile(i, j):
        return mat[j, i * LANES : (i + 1) * LANES, :]

    def put(i, j, v):
        hi = v.astype(BF16)
        lo = (v - hi.astype(F32)).astype(BF16)
        left[i * LANES : (i + 1) * LANES, j * LANES : (j + 1) * LANES] = hi
        left[depth + i * LANES : depth + (i + 1) * LANES, j * LANES : (j + 1) * LANES] = lo

    def select(base, out):
        for l in range(slots):
            at = jcode[base + l : base + l + 1, :]
            pick[:, l * LANES : (l + 1) * LANES] = jnp.where(depth_iota == at, 1.0, 0.0).astype(BF16)
        for m in range(slots // 2):
            res = jnp.dot(left[...], pick[:, m * 256 : (m + 1) * 256], preferred_element_type=F32)
            res = res[:depth] + res[depth:]
            for l in range(2):
                out[pl.ds(2 * m + l, depth, stride=slots), :] = res[:, l * LANES : (l + 1) * LANES]

    for i in range(n_tile):
        for j in range(i, n_tile):
            v = tile(i, j)
            if i == j:
                put(i, i, jnp.where(ra <= rb, v, v.T))
            else:
                put(i, j, v)
                put(j, i, v.T)
    select(0, xj)
    per_tile = LANES // slot
    for i in range(n_tile):
        for j in range(i, n_tile):
            v = tile(j, i)
            if i == j:
                diag = None
                for c in range(i * per_tile, (i + 1) * per_tile):
                    r = c // plan.halves
                    row = misc[r * cols + c][plan.folded : plan.folded + 1]
                    if per > 1 and r % per:
                        row = pltpu.roll(row, (r % per) * plan.wide, 1)
                    diag = row if diag is None else diag + row
                put(i, i, jnp.where(ra > rb, v, jnp.where(ra == rb, diag, v.T)))
            else:
                put(j, i, v)
                put(i, j, v.T)
    select(slots, zj)
    for copy in copies:
        copy.wait()

    def eight(tile_at, n):
        base = n * 8
        for s in range(8):
            total = None
            for k in range(slots):
                q = pl.multiple_of(idx[base + ((tile_at * 2 * slots + slots + k) * LANES + s)], slots)
                p = pl.multiple_of(idx[base + (tile_at * 2 * slots + k) * LANES + s], slots)
                term = xj[pl.ds(q, slots), :] * zj[pl.ds(p, slots), :]
                total = term if total is None else total + term
            acc[s * slots : (s + 1) * slots, :] = total
        out = None
        for l in range(slots):
            v = acc[pl.ds(l, 8, stride=slots), :]
            out = v if out is None else out + v
        out_ref[tile_at * LANES + base : tile_at * LANES + base + 8, :] = out

    for t in range(tiles):
        for n in range(LANES // 8):
            eight(t, n)


def send(plan, v, row_xor, col_xor):
    size = plan.cols
    pairs = []
    for r, c in itertools.product(range(plan.rows), range(plan.cols)):
        pairs.append((r * size + c, (r ^ row_xor) * size + (c ^ col_xor)))
    return lax.ppermute(v, ("row", "col"), pairs)


def gather(plan, v):
    line = [v if k == (0, 0) else send(plan, v, *k) for k in plan.far]
    stack = jnp.stack(line)
    stacks = [stack if k == (0, 0) else send(plan, stack, *k) for k in plan.near]
    return stacks + [send(plan, s, 1, 0) for s in stacks]


def schur_call(plan, stacks):
    n_tile = plan.depth // LANES
    return pl.pallas_call(
        functools.partial(main_kernel, plan, len(stacks)),
        grid=(plan.nj // LANES,),
        in_specs=[pl.BlockSpec(memory_space=pltpu.VMEM)] * len(stacks),
        out_specs=pl.BlockSpec((plan.ni, LANES), lambda c: (0, c)),
        out_shape=jax.ShapeDtypeStruct((plan.ni, plan.nj), F32),
        scratch_shapes=[
            pltpu.VMEM((plan.rows * plan.cols, EXTRA, LANES), F32),
            pltpu.VMEM((n_tile, plan.depth, LANES), F32),
            pltpu.VMEM((2 * plan.depth, plan.depth), BF16),
            pltpu.VMEM((plan.depth * plan.slots, LANES), F32),
            pltpu.VMEM((plan.depth * plan.slots, LANES), F32),
            pltpu.VMEM((plan.depth, plan.slots * LANES), BF16),
            pltpu.VMEM((plan.ni // LANES, 2 * plan.slots, LANES), I32),
            pltpu.VMEM((8 * plan.slots, LANES), F32),
            pltpu.SMEM((plan.ni * 2 * plan.slots,), I32),
            pltpu.SemaphoreType.DMA((plan.ni // LANES * 2 * plan.slots,)),
        ],
        compiler_params=pltpu.CompilerParams(vmem_limit_bytes=24 << 20),
        name="schur",
    )(*stacks)


def shards(rows, cols, moment_x, zinv, positions, entry_count):
    plan = Plan(rows, cols, moment_x.shape, positions.shape)
    packed = pl.pallas_call(
        functools.partial(pack_kernel, plan),
        out_shape=jax.ShapeDtypeStruct((plan.payload, LANES), F32),
        compiler_params=pltpu.CompilerParams(vmem_limit_bytes=4 << 20),
        name="pack",
    )(moment_x.T, zinv.T, positions.T, entry_count.reshape(1, -1))
    return schur_call(plan, gather(plan, packed))


def solution(mesh):
    return jax.shard_map(
        functools.partial(shards, mesh.shape["row"], mesh.shape["col"]),
        mesh=mesh,
        in_specs=(P("row", "col"), P("row", "col"), P(("row", "col"), None), P(("row", "col"))),
        out_specs=P("row", "col"),
        check_vma=False,
    )
```

```python
import functools
import itertools
import jax
import jax.numpy as jnp
from jax import lax
from jax.experimental import pallas as pl
from jax.experimental.pallas import tpu as pltpu
from jax.sharding import PartitionSpec as P

LANES = 128
F32, BF16, I32 = jnp.float32, jnp.bfloat16, jnp.int32
EXTRA = 8


class Plan:
    def __init__(self, rows, cols, x_shape, pos_shape):
        self.rows, self.cols = rows, cols
        self.mb, self.nb = x_shape
        self.halves = self.mb // self.nb
        self.slot = 1 << self.nb.bit_length()
        self.wide = self.halves * self.slot
        self.depth = cols * self.slot
        self.dead = self.slot - 1
        self.local, self.slots = pos_shape[0], pos_shape[1] // 2
        self.fold = LANES // self.local
        self.folded = 2 * self.slots // self.fold
        self.ni = self.local * cols
        self.nj = self.local * rows
        self.payload = self.slot + EXTRA
        row_bits, col_bits = rows.bit_length() - 1, cols.bit_length() - 1
        y_bits = col_bits // 2
        self.far = [(0, k << y_bits) for k in range(1 << (col_bits - y_bits))]
        self.near = [(i << 1, k) for i in range(1 << (row_bits - 1)) for k in range(1 << y_bits)]


def pack_kernel(plan, x_in, z_in, pos_in, cnt_in, out_ref, x_ref, z_ref, pos_ref, cnt_ref, sem):
    nb, slot, wide = plan.nb, plan.slot, plan.wide
    me_r, me_c = lax.axis_index("row"), lax.axis_index("col")
    copies = []
    for n, (src, dst) in enumerate(((x_in, x_ref), (z_in, z_ref), (pos_in, pos_ref), (cnt_in, cnt_ref))):
        copies.append(pltpu.make_async_copy(src, dst, sem.at[n]))
        copies[-1].start()
    out_ref[...] = jnp.zeros_like(out_ref)
    for copy in copies:
        copy.wait()
    a = lax.broadcasted_iota(I32, (nb, plan.mb), 0) + me_c * nb
    b = lax.broadcasted_iota(I32, (nb, plan.mb), 1) + me_r * plan.mb
    z = z_ref[...]
    mixed = jnp.where(a <= b, x_ref[...], z)
    diag = jnp.sum(jnp.where(a == b, z, 0.0), axis=0, keepdims=True)
    at = slot + plan.folded
    for h in range(plan.halves):
        out_ref[0:nb, h * slot : h * slot + nb] = mixed[:, h * nb : (h + 1) * nb]
        out_ref[at : at + 1, h * slot : h * slot + nb] = diag[:, h * nb : (h + 1) * nb]
    spots = pos_ref[...].astype(F32)
    code = spots
    for t in range(1, plan.cols):
        code = code + jnp.where(spots >= float(t * nb), float(slot - nb), 0.0)
    k = lax.broadcasted_iota(I32, code.shape, 0) % plan.slots
    code = jnp.where(k < cnt_ref[...], code, float(plan.dead))
    for g in range(plan.fold):
        piece = code[g * plan.folded : (g + 1) * plan.folded, :]
        out_ref[slot : slot + plan.folded, g * plan.local : (g + 1) * plan.local] = piece


def main_kernel(plan, n_in, *refs):
    ins, out_ref = refs[:n_in], refs[n_in]
    misc, mat, left, xj, zj, pick, ivec, acc, idx, sem = refs[n_in + 1 :]
    slot, cols, rows = plan.slot, plan.cols, plan.rows
    slots, tiles, depth = plan.slots, plan.ni // LANES, plan.depth
    me_r, me_c = lax.axis_index("row"), lax.axis_index("col")
    chunk = pl.program_id(0)
    per = LANES // plan.wide
    if per > 1:
        mat[...] = jnp.zeros_like(mat)
    near = [(core ^ i, k) for core in (0, 1) for i, k in plan.near]
    for ref, (ri, ci) in zip(ins, near):
        for n, (rf, cf) in enumerate(plan.far):
            r, c = me_r ^ (ri ^ rf), me_c ^ (ci ^ cf)
            misc[r * cols + c] = ref[n, slot:, :]
            v = ref[n, 0:slot, :]
            span = pl.ds(pl.multiple_of(c * slot, slot), slot)
            if per == 1:
                mat[r, span, :] = v
            else:
                mat[r // per, span, :] += pltpu.roll(v, (r % per) * plan.wide, 1)

    lane = lax.broadcasted_iota(I32, (plan.folded, LANES), 1) // plan.local

    def codes(first):
        got = [misc[first + e][0 : plan.folded] for e in range(plan.fold)]
        quads = []
        for g in range(plan.fold):
            quad = None
            for e in range(plan.fold):
                v = got[e]
                if e != g:
                    v = pltpu.roll(v, ((e - g) * plan.local) % LANES, 1)
                quad = v if quad is None else jnp.where(lane == e, v, quad)
            quads.append(quad)
        return jnp.concatenate(quads, axis=0).astype(I32)

    for t in range(tiles):
        ivec[t] = codes(me_r * cols + t * plan.fold) * slots
    copies = []
    for n in range(tiles * 2 * slots):
        spot = idx.at[pl.ds(n * LANES, LANES)]
        copies.append(pltpu.make_async_copy(ivec.at[n // (2 * slots), n % (2 * slots)], spot, sem.at[n]))
        copies[-1].start()
    jcode = codes(me_c * rows + chunk * plan.fold)

    depth_iota = lax.broadcasted_iota(I32, (depth, LANES), 0)
    n_tile = depth // LANES
    ra = lax.broadcasted_iota(I32, (LANES, LANES), 0)
    rb = lax.broadcasted_iota(I32, (LANES, LANES), 1)

    def tile(i, j):
        return mat[j, i * LANES : (i + 1) * LANES, :]

    def put(i, j, v):
        hi = v.astype(BF16)
        lo = (v - hi.astype(F32)).astype(BF16)
        left[i * LANES : (i + 1) * LANES, j * LANES : (j + 1) * LANES] = hi
        left[depth + i * LANES : depth + (i + 1) * LANES, j * LANES : (j + 1) * LANES] = lo

    def select(base, out):
        for l in range(slots):
            at = jcode[base + l : base + l + 1, :]
            pick[:, l * LANES : (l + 1) * LANES] = jnp.where(depth_iota == at, 1.0, 0.0).astype(BF16)
        for m in range(slots // 2):
            res = jnp.dot(left[...], pick[:, m * 256 : (m + 1) * 256], preferred_element_type=F32)
            res = res[:depth] + res[depth:]
            for l in range(2):
                out[pl.ds(2 * m + l, depth, stride=slots), :] = res[:, l * LANES : (l + 1) * LANES]

    for i in range(n_tile):
        for j in range(i, n_tile):
            v = tile(i, j)
            if i == j:
                put(i, i, jnp.where(ra <= rb, v, v.T))
            else:
                put(i, j, v)
                put(j, i, v.T)
    select(0, xj)
    per_tile = LANES // slot
    for i in range(n_tile):
        for j in range(i, n_tile):
            v = tile(j, i)
            if i == j:
                diag = None
                for c in range(i * per_tile, (i + 1) * per_tile):
                    r = c // plan.halves
                    row = misc[r * cols + c][plan.folded : plan.folded + 1]
                    if per > 1 and r % per:
                        row = pltpu.roll(row, (r % per) * plan.wide, 1)
                    diag = row if diag is None else diag + row
                put(i, i, jnp.where(ra > rb, v, jnp.where(ra == rb, diag, v.T)))
            else:
                put(j, i, v)
                put(i, j, v.T)
    select(slots, zj)
    for copy in copies:
        copy.wait()

    def eight(tile_at, n):
        base = n * 8
        for s in range(8):
            total = None
            for k in range(slots):
                q = pl.multiple_of(idx[base + ((tile_at * 2 * slots + slots + k) * LANES + s)], slots)
                p = pl.multiple_of(idx[base + (tile_at * 2 * slots + k) * LANES + s], slots)
                term = xj[pl.ds(q, slots), :] * zj[pl.ds(p, slots), :]
                total = term if total is None else total + term
            acc[s * slots : (s + 1) * slots, :] = total
        out = None
        for l in range(slots):
            v = acc[pl.ds(l, 8, stride=slots), :]
            out = v if out is None else out + v
        out_ref[tile_at * LANES + base : tile_at * LANES + base + 8, :] = out

    for t in range(tiles):
        for n in range(LANES // 8):
            eight(t, n)


def send(plan, v, row_xor, col_xor):
    size = plan.cols
    pairs = []
    for r, c in itertools.product(range(plan.rows), range(plan.cols)):
        pairs.append((r * size + c, (r ^ row_xor) * size + (c ^ col_xor)))
    return lax.ppermute(v, ("row", "col"), pairs)


def gather(plan, v):
    line = [v if k == (0, 0) else send(plan, v, *k) for k in plan.far]
    stack = jnp.stack(line)
    stacks = [stack if k == (0, 0) else send(plan, stack, *k) for k in plan.near]
    return stacks + [send(plan, s, 1, 0) for s in stacks]


def schur_call(plan, stacks):
    n_tile = plan.depth // LANES
    return pl.pallas_call(
        functools.partial(main_kernel, plan, len(stacks)),
        grid=(plan.nj // LANES,),
        in_specs=[pl.BlockSpec(memory_space=pltpu.VMEM)] * len(stacks),
        out_specs=pl.BlockSpec((plan.ni, LANES), lambda c: (0, c)),
        out_shape=jax.ShapeDtypeStruct((plan.ni, plan.nj), F32),
        scratch_shapes=[
            pltpu.VMEM((plan.rows * plan.cols, EXTRA, LANES), F32),
            pltpu.VMEM((n_tile, plan.depth, LANES), F32),
            pltpu.VMEM((2 * plan.depth, plan.depth), BF16),
            pltpu.VMEM((plan.depth * plan.slots, LANES), F32),
            pltpu.VMEM((plan.depth * plan.slots, LANES), F32),
            pltpu.VMEM((plan.depth, plan.slots * LANES), BF16),
            pltpu.VMEM((plan.ni // LANES, 2 * plan.slots, LANES), I32),
            pltpu.VMEM((8 * plan.slots, LANES), F32),
            pltpu.SMEM((plan.ni * 2 * plan.slots,), I32),
            pltpu.SemaphoreType.DMA((plan.ni // LANES * 2 * plan.slots,)),
        ],
        compiler_params=pltpu.CompilerParams(vmem_limit_bytes=24 << 20),
        name="schur",
    )(*stacks)


def shards(rows, cols, moment_x, zinv, positions, entry_count):
    plan = Plan(rows, cols, moment_x.shape, positions.shape)
    args = (moment_x.T, zinv.T, positions.T, entry_count.reshape(1, -1))
    packed = pl.pallas_call(
        functools.partial(pack_kernel, plan),
        in_specs=[pl.BlockSpec(memory_space=pltpu.HBM)] * 4,
        out_shape=jax.ShapeDtypeStruct((plan.payload, LANES), F32),
        scratch_shapes=[
            pltpu.VMEM((plan.nb, plan.mb), F32),
            pltpu.VMEM((plan.nb, plan.mb), F32),
            pltpu.VMEM((2 * plan.slots, plan.local), I32),
            pltpu.VMEM((1, plan.local), I32),
            pltpu.SemaphoreType.DMA((4,)),
        ],
        compiler_params=pltpu.CompilerParams(vmem_limit_bytes=4 << 20),
        name="pack",
    )(*[pltpu.with_memory_space_constraint(v, pltpu.HBM) for v in args])
    return schur_call(plan, gather(plan, packed))


def solution(mesh):
    return jax.shard_map(
        functools.partial(shards, mesh.shape["row"], mesh.shape["col"]),
        mesh=mesh,
        in_specs=(P("row", "col"), P("row", "col"), P(("row", "col"), None), P(("row", "col"))),
        out_specs=P("row", "col"),
        check_vma=False,
    )
```

```python
import functools
import itertools
import jax
import jax.numpy as jnp
from jax import lax
from jax.experimental import pallas as pl
from jax.experimental.pallas import tpu as pltpu
from jax.sharding import PartitionSpec as P

LANES = 128
F32, BF16, I32 = jnp.float32, jnp.bfloat16, jnp.int32
EXTRA = 8


class Plan:
    def __init__(self, rows, cols, x_shape, pos_shape):
        self.rows, self.cols = rows, cols
        self.mb, self.nb = x_shape
        self.halves = self.mb // self.nb
        self.slot = 1 << self.nb.bit_length()
        self.wide = self.halves * self.slot
        self.depth = cols * self.slot
        self.dead = self.slot - 1
        self.local, self.slots = pos_shape[0], pos_shape[1] // 2
        self.fold = LANES // self.local
        self.folded = 2 * self.slots // self.fold
        self.ni = self.local * cols
        self.nj = self.local * rows
        self.payload = self.slot + EXTRA
        row_bits, col_bits = rows.bit_length() - 1, cols.bit_length() - 1
        y_bits = col_bits // 2
        self.far = [(0, k << y_bits) for k in range(1 << (col_bits - y_bits))]
        self.near = [(i << 1, k) for i in range(1 << (row_bits - 1)) for k in range(1 << y_bits)]


def pack_kernel(plan, x_in, z_in, pos_in, cnt_in, out_ref, x_ref, z_ref, pos_ref, cnt_ref, sem):
    nb, slot, wide = plan.nb, plan.slot, plan.wide
    me_r, me_c = lax.axis_index("row"), lax.axis_index("col")
    copies = []
    for n, (src, dst) in enumerate(((x_in, x_ref), (z_in, z_ref), (pos_in, pos_ref), (cnt_in, cnt_ref))):
        copies.append(pltpu.make_async_copy(src, dst, sem.at[n]))
        copies[-1].start()
    out_ref[...] = jnp.zeros_like(out_ref)
    for copy in copies:
        copy.wait()
    a = lax.broadcasted_iota(I32, (nb, plan.mb), 0) + me_c * nb
    b = lax.broadcasted_iota(I32, (nb, plan.mb), 1) + me_r * plan.mb
    z = z_ref[...]
    mixed = jnp.where(a <= b, x_ref[...], z)
    diag = jnp.sum(jnp.where(a == b, z, 0.0), axis=0, keepdims=True)
    at = slot + plan.folded
    for h in range(plan.halves):
        out_ref[0:nb, h * slot : h * slot + nb] = mixed[:, h * nb : (h + 1) * nb]
        out_ref[at : at + 1, h * slot : h * slot + nb] = diag[:, h * nb : (h + 1) * nb]
    spots = pos_ref[...].astype(F32)
    code = spots
    for t in range(1, plan.cols):
        code = code + jnp.where(spots >= float(t * nb), float(slot - nb), 0.0)
    k = lax.broadcasted_iota(I32, code.shape, 0) % plan.slots
    code = jnp.where(k < cnt_ref[...], code, float(plan.dead))
    for g in range(plan.fold):
        piece = code[g * plan.folded : (g + 1) * plan.folded, :]
        out_ref[slot : slot + plan.folded, g * plan.local : (g + 1) * plan.local] = piece


def main_kernel(plan, n_in, *refs):
    ins, out_ref = refs[:n_in], refs[n_in]
    misc, mat, xleft, zleft, xj, zj, xpick, zpick, ivec, acc, idx, sem = refs[n_in + 1 :]
    slot, cols, rows = plan.slot, plan.cols, plan.rows
    slots, tiles, depth = plan.slots, plan.ni // LANES, plan.depth
    me_r, me_c = lax.axis_index("row"), lax.axis_index("col")
    chunk = pl.program_id(0)
    per = LANES // plan.wide
    if per > 1:
        mat[...] = jnp.zeros_like(mat)
    near = [(core ^ i, k) for core in (0, 1) for i, k in plan.near]
    for ref, (ri, ci) in zip(ins, near):
        for n, (rf, cf) in enumerate(plan.far):
            r, c = me_r ^ (ri ^ rf), me_c ^ (ci ^ cf)
            misc[r * cols + c] = ref[n, slot:, :]
            v = ref[n, 0:slot, :]
            span = pl.ds(pl.multiple_of(c * slot, slot), slot)
            if per == 1:
                mat[r, span, :] = v
            else:
                mat[r // per, span, :] += pltpu.roll(v, (r % per) * plan.wide, 1)

    lane = lax.broadcasted_iota(I32, (plan.folded, LANES), 1) // plan.local

    def codes(first):
        got = [misc[first + e][0 : plan.folded] for e in range(plan.fold)]
        quads = []
        for g in range(plan.fold):
            quad = None
            for e in range(plan.fold):
                v = got[e]
                if e != g:
                    v = pltpu.roll(v, ((e - g) * plan.local) % LANES, 1)
                quad = v if quad is None else jnp.where(lane == e, v, quad)
            quads.append(quad)
        return jnp.concatenate(quads, axis=0).astype(I32)

    for t in range(tiles):
        ivec[t] = codes(me_r * cols + t * plan.fold) * slots
    copies = []
    for n in range(tiles * 2 * slots):
        spot = idx.at[pl.ds(n * LANES, LANES)]
        copies.append(pltpu.make_async_copy(ivec.at[n // (2 * slots), n % (2 * slots)], spot, sem.at[n]))
        copies[-1].start()
    jcode = codes(me_c * rows + chunk * plan.fold)

    depth_iota = lax.broadcasted_iota(I32, (depth, LANES), 0)
    n_tile = depth // LANES
    ra = lax.broadcasted_iota(I32, (LANES, LANES), 0)
    rb = lax.broadcasted_iota(I32, (LANES, LANES), 1)

    def tile(i, j):
        return mat[j, i * LANES : (i + 1) * LANES, :]

    def put(left, i, j, v):
        hi = v.astype(BF16)
        lo = (v - hi.astype(F32)).astype(BF16)
        left[i * LANES : (i + 1) * LANES, j * LANES : (j + 1) * LANES] = hi
        left[depth + i * LANES : depth + (i + 1) * LANES, j * LANES : (j + 1) * LANES] = lo

    def mark(base, pick):
        for l in range(slots):
            at = jcode[base + l : base + l + 1, :]
            pick[:, l * LANES : (l + 1) * LANES] = jnp.where(depth_iota == at, 1.0, 0.0).astype(BF16)

    def select(left, pick, out):
        for m in range(slots // 2):
            res = jnp.dot(left[...], pick[:, m * 256 : (m + 1) * 256], preferred_element_type=F32)
            res = res[:depth] + res[depth:]
            for l in range(2):
                out[pl.ds(2 * m + l, depth, stride=slots), :] = res[:, l * LANES : (l + 1) * LANES]

    mark(0, xpick)
    for i in range(n_tile):
        for j in range(i, n_tile):
            v = tile(i, j)
            if i == j:
                put(xleft, i, i, jnp.where(ra <= rb, v, v.T))
            else:
                put(xleft, i, j, v)
                put(xleft, j, i, v.T)
    select(xleft, xpick, xj)
    mark(slots, zpick)
    per_tile = LANES // slot
    for i in range(n_tile):
        for j in range(i, n_tile):
            v = tile(j, i)
            if i == j:
                diag = None
                for c in range(i * per_tile, (i + 1) * per_tile):
                    r = c // plan.halves
                    row = misc[r * cols + c][plan.folded : plan.folded + 1]
                    if per > 1 and r % per:
                        row = pltpu.roll(row, (r % per) * plan.wide, 1)
                    diag = row if diag is None else diag + row
                put(zleft, i, i, jnp.where(ra > rb, v, jnp.where(ra == rb, diag, v.T)))
            else:
                put(zleft, j, i, v)
                put(zleft, i, j, v.T)
    select(zleft, zpick, zj)
    for copy in copies:
        copy.wait()

    def eight(tile_at, n):
        base = n * 8
        for s in range(8):
            total = None
            for k in range(slots):
                q = pl.multiple_of(idx[base + ((tile_at * 2 * slots + slots + k) * LANES + s)], slots)
                p = pl.multiple_of(idx[base + (tile_at * 2 * slots + k) * LANES + s], slots)
                term = xj[pl.ds(q, slots), :] * zj[pl.ds(p, slots), :]
                total = term if total is None else total + term
            acc[s * slots : (s + 1) * slots, :] = total
        out = None
        for l in range(slots):
            v = acc[pl.ds(l, 8, stride=slots), :]
            out = v if out is None else out + v
        out_ref[tile_at * LANES + base : tile_at * LANES + base + 8, :] = out

    for t in range(tiles):
        for n in range(LANES // 8):
            eight(t, n)


def send(plan, v, row_xor, col_xor):
    size = plan.cols
    pairs = []
    for r, c in itertools.product(range(plan.rows), range(plan.cols)):
        pairs.append((r * size + c, (r ^ row_xor) * size + (c ^ col_xor)))
    return lax.ppermute(v, ("row", "col"), pairs)


def gather(plan, v):
    line = [v if k == (0, 0) else send(plan, v, *k) for k in plan.far]
    stack = jnp.stack(line)
    stacks = [stack if k == (0, 0) else send(plan, stack, *k) for k in plan.near]
    return stacks + [send(plan, s, 1, 0) for s in stacks]


def schur_call(plan, stacks):
    n_tile = plan.depth // LANES
    return pl.pallas_call(
        functools.partial(main_kernel, plan, len(stacks)),
        grid=(plan.nj // LANES,),
        in_specs=[pl.BlockSpec(memory_space=pltpu.VMEM)] * len(stacks),
        out_specs=pl.BlockSpec((plan.ni, LANES), lambda c: (0, c)),
        out_shape=jax.ShapeDtypeStruct((plan.ni, plan.nj), F32),
        scratch_shapes=[
            pltpu.VMEM((plan.rows * plan.cols, EXTRA, LANES), F32),
            pltpu.VMEM((n_tile, plan.depth, LANES), F32),
            pltpu.VMEM((2 * plan.depth, plan.depth), BF16),
            pltpu.VMEM((2 * plan.depth, plan.depth), BF16),
            pltpu.VMEM((plan.depth * plan.slots, LANES), F32),
            pltpu.VMEM((plan.depth * plan.slots, LANES), F32),
            pltpu.VMEM((plan.depth, plan.slots * LANES), BF16),
            pltpu.VMEM((plan.depth, plan.slots * LANES), BF16),
            pltpu.VMEM((plan.ni // LANES, 2 * plan.slots, LANES), I32),
            pltpu.VMEM((8 * plan.slots, LANES), F32),
            pltpu.SMEM((plan.ni * 2 * plan.slots,), I32),
            pltpu.SemaphoreType.DMA((plan.ni // LANES * 2 * plan.slots,)),
        ],
        compiler_params=pltpu.CompilerParams(vmem_limit_bytes=24 << 20),
        name="schur",
    )(*stacks)


def shards(rows, cols, moment_x, zinv, positions, entry_count):
    plan = Plan(rows, cols, moment_x.shape, positions.shape)
    args = (moment_x.T, zinv.T, positions.T, entry_count.reshape(1, -1))
    packed = pl.pallas_call(
        functools.partial(pack_kernel, plan),
        in_specs=[pl.BlockSpec(memory_space=pltpu.HBM)] * 4,
        out_shape=jax.ShapeDtypeStruct((plan.payload, LANES), F32),
        scratch_shapes=[
            pltpu.VMEM((plan.nb, plan.mb), F32),
            pltpu.VMEM((plan.nb, plan.mb), F32),
            pltpu.VMEM((2 * plan.slots, plan.local), I32),
            pltpu.VMEM((1, plan.local), I32),
            pltpu.SemaphoreType.DMA((4,)),
        ],
        compiler_params=pltpu.CompilerParams(vmem_limit_bytes=4 << 20),
        name="pack",
    )(*[pltpu.with_memory_space_constraint(v, pltpu.HBM) for v in args])
    return schur_call(plan, gather(plan, packed))


def solution(mesh):
    return jax.shard_map(
        functools.partial(shards, mesh.shape["row"], mesh.shape["col"]),
        mesh=mesh,
        in_specs=(P("row", "col"), P("row", "col"), P(("row", "col"), None), P(("row", "col"))),
        out_specs=P("row", "col"),
        check_vma=False,
    )
```

```python
import functools
import itertools
import jax
import jax.numpy as jnp
from jax import lax
from jax.experimental import pallas as pl
from jax.experimental.pallas import tpu as pltpu
from jax.sharding import PartitionSpec as P

LANES = 128
F32, BF16, I32 = jnp.float32, jnp.bfloat16, jnp.int32
EXTRA = 8


class Plan:
    def __init__(self, rows, cols, x_shape, pos_shape):
        self.rows, self.cols = rows, cols
        self.mb, self.nb = x_shape
        self.halves = self.mb // self.nb
        self.slot = 1 << self.nb.bit_length()
        self.wide = self.halves * self.slot
        self.depth = cols * self.slot
        self.dead = self.slot - 1
        self.local, self.slots = pos_shape[0], pos_shape[1] // 2
        self.fold = LANES // self.local
        self.folded = 2 * self.slots // self.fold
        self.ni = self.local * cols
        self.nj = self.local * rows
        self.payload = self.slot + EXTRA
        row_bits, col_bits = rows.bit_length() - 1, cols.bit_length() - 1
        y_bits = col_bits // 2
        self.far = [(0, k << y_bits) for k in range(1 << (col_bits - y_bits))]
        self.near = [(i << 1, k) for i in range(1 << (row_bits - 1)) for k in range(1 << y_bits)]


def pack_kernel(plan, x_in, z_in, pos_in, cnt_in, out_ref, x_ref, z_ref, pos_ref, cnt_ref, sem):
    nb, slot, wide = plan.nb, plan.slot, plan.wide
    me_r, me_c = lax.axis_index("row"), lax.axis_index("col")
    copies = []
    for n, (src, dst) in enumerate(((x_in, x_ref), (z_in, z_ref), (pos_in, pos_ref), (cnt_in, cnt_ref))):
        copies.append(pltpu.make_async_copy(src, dst, sem.at[n]))
        copies[-1].start()
    out_ref[...] = jnp.zeros_like(out_ref)
    for copy in copies:
        copy.wait()
    a = lax.broadcasted_iota(I32, (nb, plan.mb), 0) + me_c * nb
    b = lax.broadcasted_iota(I32, (nb, plan.mb), 1) + me_r * plan.mb
    z = z_ref[...]
    mixed = jnp.where(a <= b, x_ref[...], z)
    diag = jnp.sum(jnp.where(a == b, z, 0.0), axis=0, keepdims=True)
    at = slot + plan.folded
    for h in range(plan.halves):
        out_ref[0:nb, h * slot : h * slot + nb] = mixed[:, h * nb : (h + 1) * nb]
        out_ref[at : at + 1, h * slot : h * slot + nb] = diag[:, h * nb : (h + 1) * nb]
    spots = pos_ref[...].astype(F32)
    code = spots
    for t in range(1, plan.cols):
        code = code + jnp.where(spots >= float(t * nb), float(slot - nb), 0.0)
    k = lax.broadcasted_iota(I32, code.shape, 0) % plan.slots
    code = jnp.where(k < cnt_ref[...], code, float(plan.dead))
    for g in range(plan.fold):
        piece = code[g * plan.folded : (g + 1) * plan.folded, :]
        out_ref[slot : slot + plan.folded, g * plan.local : (g + 1) * plan.local] = piece


def main_kernel(plan, n_in, *refs):
    ins, out_hbm = refs[:n_in], refs[n_in]
    out_ref, osem, misc, mat, xleft, zleft, xj, zj, xpick, zpick, ivec, acc, idx, sem = refs[n_in + 1 :]
    slot, cols, rows = plan.slot, plan.cols, plan.rows
    slots, tiles, depth = plan.slots, plan.ni // LANES, plan.depth
    me_r, me_c = lax.axis_index("row"), lax.axis_index("col")
    chunk = pl.program_id(0)
    per = LANES // plan.wide
    if per > 1:
        mat[...] = jnp.zeros_like(mat)
    near = [(core ^ i, k) for core in (0, 1) for i, k in plan.near]
    for ref, (ri, ci) in zip(ins, near):
        for n, (rf, cf) in enumerate(plan.far):
            r, c = me_r ^ (ri ^ rf), me_c ^ (ci ^ cf)
            misc[r * cols + c] = ref[n, slot:, :]
            v = ref[n, 0:slot, :]
            span = pl.ds(pl.multiple_of(c * slot, slot), slot)
            if per == 1:
                mat[r, span, :] = v
            else:
                mat[r // per, span, :] += pltpu.roll(v, (r % per) * plan.wide, 1)

    lane = lax.broadcasted_iota(I32, (plan.folded, LANES), 1) // plan.local

    def codes(first):
        got = [misc[first + e][0 : plan.folded] for e in range(plan.fold)]
        quads = []
        for g in range(plan.fold):
            quad = None
            for e in range(plan.fold):
                v = got[e]
                if e != g:
                    v = pltpu.roll(v, ((e - g) * plan.local) % LANES, 1)
                quad = v if quad is None else jnp.where(lane == e, v, quad)
            quads.append(quad)
        return jnp.concatenate(quads, axis=0).astype(I32)

    copy = pltpu.make_async_copy(ivec, idx, sem)

    @pl.when(me_r >= 0)
    def _():
        for t in range(tiles):
            ivec[t] = codes(me_r * cols + t * plan.fold) * slots
        copy.start()

    jcode = codes(me_c * rows + chunk * plan.fold)

    depth_iota = lax.broadcasted_iota(I32, (depth, LANES), 0)
    n_tile = depth // LANES
    ra = lax.broadcasted_iota(I32, (LANES, LANES), 0)
    rb = lax.broadcasted_iota(I32, (LANES, LANES), 1)

    def tile(i, j):
        return mat[j, i * LANES : (i + 1) * LANES, :]

    def put(left, i, j, v):
        hi = v.astype(BF16)
        lo = (v - hi.astype(F32)).astype(BF16)
        left[i * LANES : (i + 1) * LANES, j * LANES : (j + 1) * LANES] = hi
        left[depth + i * LANES : depth + (i + 1) * LANES, j * LANES : (j + 1) * LANES] = lo

    def mark(base, pick):
        for l in range(slots):
            at = jcode[base + l : base + l + 1, :]
            pick[:, l * LANES : (l + 1) * LANES] = jnp.where(depth_iota == at, 1.0, 0.0).astype(BF16)

    def select(left, pick, out):
        for m in range(slots // 2):
            res = jnp.dot(left[...], pick[:, m * 256 : (m + 1) * 256], preferred_element_type=F32)
            res = res[:depth] + res[depth:]
            for l in range(2):
                out[pl.ds(2 * m + l, depth, stride=slots), :] = res[:, l * LANES : (l + 1) * LANES]

    mark(0, xpick)
    for i in range(n_tile):
        for j in range(i, n_tile):
            v = tile(i, j)
            if i == j:
                put(xleft, i, i, jnp.where(ra <= rb, v, v.T))
            else:
                put(xleft, i, j, v)
                put(xleft, j, i, v.T)
    select(xleft, xpick, xj)
    mark(slots, zpick)
    per_tile = LANES // slot
    for i in range(n_tile):
        for j in range(i, n_tile):
            v = tile(j, i)
            if i == j:
                diag = None
                for c in range(i * per_tile, (i + 1) * per_tile):
                    r = c // plan.halves
                    row = misc[r * cols + c][plan.folded : plan.folded + 1]
                    if per > 1 and r % per:
                        row = pltpu.roll(row, (r % per) * plan.wide, 1)
                    diag = row if diag is None else diag + row
                put(zleft, i, i, jnp.where(ra > rb, v, jnp.where(ra == rb, diag, v.T)))
            else:
                put(zleft, j, i, v)
                put(zleft, i, j, v.T)
    select(zleft, zpick, zj)
    copy.wait()

    def eight(tile_at, n):
        base = n * 8
        for s in range(8):
            total = None
            for k in range(slots):
                q = pl.multiple_of(idx[tile_at, slots + k, base + s], slots)
                p = pl.multiple_of(idx[tile_at, k, base + s], slots)
                term = xj[pl.ds(q, slots), :] * zj[pl.ds(p, slots), :]
                total = term if total is None else total + term
            acc[s * slots : (s + 1) * slots, :] = total
        out = None
        for l in range(slots):
            v = acc[pl.ds(l, 8, stride=slots), :]
            out = v if out is None else out + v
        out_ref[tile_at * LANES + base : tile_at * LANES + base + 8, :] = out

    outs = []
    for t in range(tiles):
        for n in range(LANES // 8):
            eight(t, n)
        span = pl.ds(t * LANES, LANES)
        there = out_hbm.at[span, pl.ds(pl.multiple_of(chunk * LANES, LANES), LANES)]
        outs.append(pltpu.make_async_copy(out_ref.at[span], there, osem.at[t]))
        outs[-1].start()
    for copy in outs:
        copy.wait()


def send(plan, v, row_xor, col_xor):
    size = plan.cols
    pairs = []
    for r, c in itertools.product(range(plan.rows), range(plan.cols)):
        pairs.append((r * size + c, (r ^ row_xor) * size + (c ^ col_xor)))
    return lax.ppermute(v, ("row", "col"), pairs)


def gather(plan, v):
    line = [v if k == (0, 0) else send(plan, v, *k) for k in plan.far]
    stack = jnp.stack(line)
    stacks = [stack if k == (0, 0) else send(plan, stack, *k) for k in plan.near]
    return stacks + [send(plan, s, 1, 0) for s in stacks]


def schur_call(plan, stacks):
    n_tile = plan.depth // LANES
    return pl.pallas_call(
        functools.partial(main_kernel, plan, len(stacks)),
        grid=(plan.nj // LANES,),
        in_specs=[pl.BlockSpec(memory_space=pltpu.VMEM)] * len(stacks),
        out_specs=pl.BlockSpec(memory_space=pltpu.HBM),
        out_shape=jax.ShapeDtypeStruct((plan.ni, plan.nj), F32),
        scratch_shapes=[
            pltpu.VMEM((plan.ni, LANES), F32),
            pltpu.SemaphoreType.DMA((plan.ni // LANES,)),
            pltpu.VMEM((plan.rows * plan.cols, EXTRA, LANES), F32),
            pltpu.VMEM((n_tile, plan.depth, LANES), F32),
            pltpu.VMEM((2 * plan.depth, plan.depth), BF16),
            pltpu.VMEM((2 * plan.depth, plan.depth), BF16),
            pltpu.VMEM((plan.depth * plan.slots, LANES), F32),
            pltpu.VMEM((plan.depth * plan.slots, LANES), F32),
            pltpu.VMEM((plan.depth, plan.slots * LANES), BF16),
            pltpu.VMEM((plan.depth, plan.slots * LANES), BF16),
            pltpu.VMEM((plan.ni // LANES, 2 * plan.slots, LANES), I32),
            pltpu.VMEM((8 * plan.slots, LANES), F32),
            pltpu.SMEM((plan.ni // LANES, 2 * plan.slots, LANES), I32),
            pltpu.SemaphoreType.DMA,
        ],
        compiler_params=pltpu.CompilerParams(vmem_limit_bytes=24 << 20),
        name="schur",
    )(*stacks)


def shards(rows, cols, moment_x, zinv, positions, entry_count):
    plan = Plan(rows, cols, moment_x.shape, positions.shape)
    args = (moment_x.T, zinv.T, positions.T, entry_count.reshape(1, -1))
    packed = pl.pallas_call(
        functools.partial(pack_kernel, plan),
        in_specs=[pl.BlockSpec(memory_space=pltpu.HBM)] * 4,
        out_shape=jax.ShapeDtypeStruct((plan.payload, LANES), F32),
        scratch_shapes=[
            pltpu.VMEM((plan.nb, plan.mb), F32),
            pltpu.VMEM((plan.nb, plan.mb), F32),
            pltpu.VMEM((2 * plan.slots, plan.local), I32),
            pltpu.VMEM((1, plan.local), I32),
            pltpu.SemaphoreType.DMA((4,)),
        ],
        compiler_params=pltpu.CompilerParams(vmem_limit_bytes=4 << 20),
        name="pack",
    )(*[pltpu.with_memory_space_constraint(v, pltpu.HBM) for v in args])
    return schur_call(plan, gather(plan, packed))


def solution(mesh):
    return jax.shard_map(
        functools.partial(shards, mesh.shape["row"], mesh.shape["col"]),
        mesh=mesh,
        in_specs=(P("row", "col"), P("row", "col"), P(("row", "col"), None), P(("row", "col"))),
        out_specs=P("row", "col"),
        check_vma=False,
    )
```

```python
import functools
import itertools
import jax
import jax.numpy as jnp
from jax import lax
from jax.experimental import pallas as pl
from jax.experimental.pallas import tpu as pltpu
from jax.sharding import PartitionSpec as P

LANES = 128
F32, BF16, I32 = jnp.float32, jnp.bfloat16, jnp.int32
EXTRA = 8


class Plan:
    def __init__(self, rows, cols, x_shape, pos_shape):
        self.rows, self.cols = rows, cols
        self.mb, self.nb = x_shape
        self.halves = self.mb // self.nb
        self.slot = 1 << self.nb.bit_length()
        self.wide = self.halves * self.slot
        self.depth = cols * self.slot
        self.dead = self.slot - 1
        self.local, self.slots = pos_shape[0], pos_shape[1] // 2
        self.fold = LANES // self.local
        self.folded = 2 * self.slots // self.fold
        self.ni = self.local * cols
        self.nj = self.local * rows
        self.payload = self.slot + EXTRA
        row_bits, col_bits = rows.bit_length() - 1, cols.bit_length() - 1
        y_bits = col_bits // 2
        self.far = [(0, k << y_bits) for k in range(1 << (col_bits - y_bits))]
        self.near = [(i << 1, k) for i in range(1 << (row_bits - 1)) for k in range(1 << y_bits)]


def pack_kernel(plan, x_in, z_in, pos_in, cnt_in, out_ref, x_ref, z_ref, pos_ref, cnt_ref, sem):
    nb, slot, wide = plan.nb, plan.slot, plan.wide
    me_r, me_c = lax.axis_index("row"), lax.axis_index("col")
    copies = []
    for n, (src, dst) in enumerate(((x_in, x_ref), (z_in, z_ref), (pos_in, pos_ref), (cnt_in, cnt_ref))):
        copies.append(pltpu.make_async_copy(src, dst, sem.at[n]))
        copies[-1].start()
    out_ref[...] = jnp.zeros_like(out_ref)
    for copy in copies:
        copy.wait()
    a = lax.broadcasted_iota(I32, (nb, plan.mb), 0) + me_c * nb
    b = lax.broadcasted_iota(I32, (nb, plan.mb), 1) + me_r * plan.mb
    z = z_ref[...]
    mixed = jnp.where(a <= b, x_ref[...], z)
    diag = jnp.sum(jnp.where(a == b, z, 0.0), axis=0, keepdims=True)
    at = slot + plan.folded
    for h in range(plan.halves):
        out_ref[0:nb, h * slot : h * slot + nb] = mixed[:, h * nb : (h + 1) * nb]
        out_ref[at : at + 1, h * slot : h * slot + nb] = diag[:, h * nb : (h + 1) * nb]
    spots = pos_ref[...].astype(F32)
    code = spots
    for t in range(1, plan.cols):
        code = code + jnp.where(spots >= float(t * nb), float(slot - nb), 0.0)
    k = lax.broadcasted_iota(I32, code.shape, 0) % plan.slots
    code = jnp.where(k < cnt_ref[...], code, float(plan.dead))
    for g in range(plan.fold):
        piece = code[g * plan.folded : (g + 1) * plan.folded, :]
        out_ref[slot : slot + plan.folded, g * plan.local : (g + 1) * plan.local] = piece


def main_kernel(plan, n_in, *refs):
    ins, out_hbm = refs[:n_in], refs[n_in]
    out_ref, osem, misc, mat, left, zrow, zgot, xj, zj, pick, ivec, jvec, acc, idx, jdx, sem = refs[n_in + 1 :]
    slot, cols, rows = plan.slot, plan.cols, plan.rows
    slots, tiles, depth = plan.slots, plan.ni // LANES, plan.depth
    me_r, me_c = lax.axis_index("row"), lax.axis_index("col")
    chunk = pl.program_id(0)
    per = LANES // plan.wide
    if per > 1:
        mat[...] = jnp.zeros_like(mat)
    near = [(core ^ i, k) for core in (0, 1) for i, k in plan.near]
    for ref, (ri, ci) in zip(ins, near):
        for n, (rf, cf) in enumerate(plan.far):
            r, c = me_r ^ (ri ^ rf), me_c ^ (ci ^ cf)
            misc[r * cols + c] = ref[n, slot:, :]
            v = ref[n, 0:slot, :]
            span = pl.ds(pl.multiple_of(c * slot, slot), slot)
            if per == 1:
                mat[r, span, :] = v
            else:
                mat[r // per, span, :] += pltpu.roll(v, (r % per) * plan.wide, 1)

    lane = lax.broadcasted_iota(I32, (plan.folded, LANES), 1) // plan.local

    def codes(first):
        got = [misc[first + e][0 : plan.folded] for e in range(plan.fold)]
        quads = []
        for g in range(plan.fold):
            quad = None
            for e in range(plan.fold):
                v = got[e]
                if e != g:
                    v = pltpu.roll(v, ((e - g) * plan.local) % LANES, 1)
                quad = v if quad is None else jnp.where(lane == e, v, quad)
            quads.append(quad)
        return jnp.concatenate(quads, axis=0).astype(I32)

    n_tile = depth // LANES
    jcode = codes(me_c * rows + chunk * plan.fold)
    icopy = pltpu.make_async_copy(ivec, idx, sem.at[0])
    jcopy = pltpu.make_async_copy(jvec, jdx, sem.at[1])

    @pl.when(me_r >= 0)
    def _():
        jvec[...] = codes(me_c * rows + chunk * plan.fold)[slots:] * n_tile
        jcopy.start()
        for t in range(tiles):
            ivec[t] = codes(me_r * cols + t * plan.fold) * slots
        icopy.start()

    depth_iota = lax.broadcasted_iota(I32, (depth, LANES), 0)
    ra = lax.broadcasted_iota(I32, (LANES, LANES), 0)
    rb = lax.broadcasted_iota(I32, (LANES, LANES), 1)

    def tile(i, j):
        return mat[j, i * LANES : (i + 1) * LANES, :]

    def put_x(i, j, v):
        hi = v.astype(BF16)
        lo = (v - hi.astype(F32)).astype(BF16)
        left[i * LANES : (i + 1) * LANES, j * LANES : (j + 1) * LANES] = hi
        left[depth + i * LANES : depth + (i + 1) * LANES, j * LANES : (j + 1) * LANES] = lo

    def put_z(i, j, v):
        zrow[pl.ds(8 + i * LANES * n_tile + j, LANES, stride=n_tile), :] = v

    per_tile = LANES // slot
    for i in range(n_tile):
        for j in range(i, n_tile):
            v = tile(j, i)
            if i == j:
                diag = None
                for c in range(i * per_tile, (i + 1) * per_tile):
                    r = c // plan.halves
                    row = misc[r * cols + c][plan.folded : plan.folded + 1]
                    if per > 1 and r % per:
                        row = pltpu.roll(row, (r % per) * plan.wide, 1)
                    diag = row if diag is None else diag + row
                put_z(i, i, jnp.where(ra > rb, v, jnp.where(ra == rb, diag, v.T)))
            else:
                put_z(j, i, v)
                put_z(i, j, v.T)
    for l in range(slots):
        at = jcode[l : l + 1, :]
        pick[:, l * LANES : (l + 1) * LANES] = jnp.where(depth_iota == at, 1.0, 0.0).astype(BF16)
    for i in range(n_tile):
        for j in range(i, n_tile):
            v = tile(i, j)
            if i == j:
                put_x(i, i, jnp.where(ra <= rb, v, v.T))
            else:
                put_x(i, j, v)
                put_x(j, i, v.T)

    group = lax.broadcasted_iota(I32, (8, LANES), 0) // n_tile
    jcopy.wait()

    def gather_rows(l):
        for j in range(0, LANES, 8 // n_tile):
            both = None
            for e in range(8 // n_tile):
                at = pl.multiple_of(jdx[l, j + e], n_tile)
                v = zrow[pl.ds(at + (8 - e * n_tile), 8), :]
                both = v if both is None else jnp.where(group == e, v, both)
            base = (l * LANES + j) * n_tile
            zgot[base : base + 8, :] = both
        for s in range(n_tile):
            v = zgot[pl.ds(l * LANES * n_tile + s, LANES, stride=n_tile), :]
            zj[pl.ds(s * LANES * slots + l, LANES, stride=slots), :] = v.T

    for m in range(slots // 2):
        res = jnp.dot(left[...], pick[:, m * 256 : (m + 1) * 256], preferred_element_type=F32)
        res = res[:depth] + res[depth:]
        for l in range(2):
            xj[pl.ds(2 * m + l, depth, stride=slots), :] = res[:, l * LANES : (l + 1) * LANES]
    for l in range(slots):
        gather_rows(l)
    icopy.wait()

    def eight(tile_at, n):
        base = n * 8
        for s in range(8):
            total = None
            for k in range(slots):
                q = pl.multiple_of(idx[tile_at, slots + k, base + s], slots)
                p = pl.multiple_of(idx[tile_at, k, base + s], slots)
                term = xj[pl.ds(q, slots), :] * zj[pl.ds(p, slots), :]
                total = term if total is None else total + term
            acc[s * slots : (s + 1) * slots, :] = total
        out = None
        for l in range(slots):
            v = acc[pl.ds(l, 8, stride=slots), :]
            out = v if out is None else out + v
        out_ref[tile_at * LANES + base : tile_at * LANES + base + 8, :] = out

    outs = []
    for t in range(tiles):
        for n in range(LANES // 8):
            eight(t, n)
        span = pl.ds(t * LANES, LANES)
        there = out_hbm.at[span, pl.ds(pl.multiple_of(chunk * LANES, LANES), LANES)]
        outs.append(pltpu.make_async_copy(out_ref.at[span], there, osem.at[t]))
        outs[-1].start()
    for copy in outs:
        copy.wait()


def send(plan, v, row_xor, col_xor):
    size = plan.cols
    pairs = []
    for r, c in itertools.product(range(plan.rows), range(plan.cols)):
        pairs.append((r * size + c, (r ^ row_xor) * size + (c ^ col_xor)))
    return lax.ppermute(v, ("row", "col"), pairs)


def gather(plan, v):
    line = [v if k == (0, 0) else send(plan, v, *k) for k in plan.far]
    stack = jnp.stack(line)
    stacks = [stack if k == (0, 0) else send(plan, stack, *k) for k in plan.near]
    return stacks + [send(plan, s, 1, 0) for s in stacks]


def schur_call(plan, stacks):
    n_tile = plan.depth // LANES
    return pl.pallas_call(
        functools.partial(main_kernel, plan, len(stacks)),
        grid=(plan.nj // LANES,),
        in_specs=[pl.BlockSpec(memory_space=pltpu.VMEM)] * len(stacks),
        out_specs=pl.BlockSpec(memory_space=pltpu.HBM),
        out_shape=jax.ShapeDtypeStruct((plan.ni, plan.nj), F32),
        scratch_shapes=[
            pltpu.VMEM((plan.ni, LANES), F32),
            pltpu.SemaphoreType.DMA((plan.ni // LANES,)),
            pltpu.VMEM((plan.rows * plan.cols, EXTRA, LANES), F32),
            pltpu.VMEM((n_tile, plan.depth, LANES), F32),
            pltpu.VMEM((2 * plan.depth, plan.depth), BF16),
            pltpu.VMEM((plan.depth * n_tile + 16, LANES), F32),
            pltpu.VMEM((plan.slots * LANES * n_tile, LANES), F32),
            pltpu.VMEM((plan.depth * plan.slots, LANES), F32),
            pltpu.VMEM((plan.depth * plan.slots, LANES), F32),
            pltpu.VMEM((plan.depth, plan.slots * LANES), BF16),
            pltpu.VMEM((plan.ni // LANES, 2 * plan.slots, LANES), I32),
            pltpu.VMEM((plan.slots, LANES), I32),
            pltpu.VMEM((8 * plan.slots, LANES), F32),
            pltpu.SMEM((plan.ni // LANES, 2 * plan.slots, LANES), I32),
            pltpu.SMEM((plan.slots, LANES), I32),
            pltpu.SemaphoreType.DMA((2,)),
        ],
        compiler_params=pltpu.CompilerParams(vmem_limit_bytes=24 << 20),
        name="schur",
    )(*stacks)


def shards(rows, cols, moment_x, zinv, positions, entry_count):
    plan = Plan(rows, cols, moment_x.shape, positions.shape)
    args = (moment_x.T, zinv.T, positions.T, entry_count.reshape(1, -1))
    packed = pl.pallas_call(
        functools.partial(pack_kernel, plan),
        in_specs=[pl.BlockSpec(memory_space=pltpu.HBM)] * 4,
        out_shape=jax.ShapeDtypeStruct((plan.payload, LANES), F32),
        scratch_shapes=[
            pltpu.VMEM((plan.nb, plan.mb), F32),
            pltpu.VMEM((plan.nb, plan.mb), F32),
            pltpu.VMEM((2 * plan.slots, plan.local), I32),
            pltpu.VMEM((1, plan.local), I32),
            pltpu.SemaphoreType.DMA((4,)),
        ],
        compiler_params=pltpu.CompilerParams(vmem_limit_bytes=4 << 20),
        name="pack",
    )(*[pltpu.with_memory_space_constraint(v, pltpu.HBM) for v in args])
    return schur_call(plan, gather(plan, packed))


def solution(mesh):
    return jax.shard_map(
        functools.partial(shards, mesh.shape["row"], mesh.shape["col"]),
        mesh=mesh,
        in_specs=(P("row", "col"), P("row", "col"), P(("row", "col"), None), P(("row", "col"))),
        out_specs=P("row", "col"),
        check_vma=False,
    )
```

```python
import functools
import itertools
import jax
import jax.numpy as jnp
from jax import lax
from jax.experimental import pallas as pl
from jax.experimental.pallas import tpu as pltpu
from jax.sharding import PartitionSpec as P

LANES = 128
F32, BF16, I32 = jnp.float32, jnp.bfloat16, jnp.int32
EXTRA = 8


class Plan:
    def __init__(self, rows, cols, x_shape, pos_shape):
        self.rows, self.cols = rows, cols
        self.mb, self.nb = x_shape
        self.halves = self.mb // self.nb
        self.slot = 1 << self.nb.bit_length()
        self.wide = self.halves * self.slot
        self.depth = cols * self.slot
        self.dead = self.slot - 1
        self.local, self.slots = pos_shape[0], pos_shape[1] // 2
        self.fold = LANES // self.local
        self.folded = 2 * self.slots // self.fold
        self.ni = self.local * cols
        self.nj = self.local * rows
        self.used = self.nb + self.folded
        self.payload = -(-max(self.slot, self.used) // 8) * 8
        row_bits, col_bits = rows.bit_length() - 1, cols.bit_length() - 1
        y_bits = col_bits // 2
        self.far = [(0, k << y_bits) for k in range(1 << (col_bits - y_bits))]
        self.near = [(i << 1, k) for i in range(1 << (row_bits - 1)) for k in range(1 << y_bits)]


def pack_kernel(plan, x_in, z_in, pos_in, cnt_in, out_ref, x_ref, z_ref, pos_ref, cnt_ref, sem):
    nb, slot, wide = plan.nb, plan.slot, plan.wide
    me_r, me_c = lax.axis_index("row"), lax.axis_index("col")
    copies = []
    for n, (src, dst) in enumerate(((x_in, x_ref), (z_in, z_ref), (pos_in, pos_ref), (cnt_in, cnt_ref))):
        copies.append(pltpu.make_async_copy(src, dst, sem.at[n]))
        copies[-1].start()
    out_ref[...] = jnp.zeros_like(out_ref)
    for copy in copies:
        copy.wait()
    a = lax.broadcasted_iota(I32, (nb, plan.mb), 0) + me_c * nb
    b = lax.broadcasted_iota(I32, (nb, plan.mb), 1) + me_r * plan.mb
    z = z_ref[...]
    mixed = jnp.where(a <= b, x_ref[...], z)
    diag = jnp.sum(jnp.where(a == b, z, 0.0), axis=1, keepdims=True)
    for h in range(plan.halves):
        out_ref[0:nb, h * slot : h * slot + nb] = mixed[:, h * nb : (h + 1) * nb]
    out_ref[0:nb, nb : nb + 1] = diag
    spots = pos_ref[...].astype(F32)
    code = spots
    for t in range(1, plan.cols):
        code = code + jnp.where(spots >= float(t * nb), float(slot - nb), 0.0)
    k = lax.broadcasted_iota(I32, code.shape, 0) % plan.slots
    code = jnp.where(k < cnt_ref[...], code, float(plan.dead))
    for g in range(plan.fold):
        piece = code[g * plan.folded : (g + 1) * plan.folded, :]
        out_ref[nb : nb + plan.folded, g * plan.local : (g + 1) * plan.local] = piece


def main_kernel(plan, n_in, *refs):
    ins, out_hbm = refs[:n_in], refs[n_in]
    out_ref, osem, misc, mat, left, zrow, zgot, xj, zj, pick, ivec, jvec, acc, idx, jdx, sem = refs[n_in + 1 :]
    slot, cols, rows = plan.slot, plan.cols, plan.rows
    slots, tiles, depth = plan.slots, plan.ni // LANES, plan.depth
    me_r, me_c = lax.axis_index("row"), lax.axis_index("col")
    chunk = pl.program_id(0)
    per = LANES // plan.wide
    if per > 1:
        mat[...] = jnp.zeros_like(mat)
    live_row = lax.broadcasted_iota(I32, (slot, LANES), 0) < plan.nb
    near = [(core ^ i, k) for core in (0, 1) for i, k in plan.near]
    for ref, (ri, ci) in zip(ins, near):
        for n, (rf, cf) in enumerate(plan.far):
            r, c = me_r ^ (ri ^ rf), me_c ^ (ci ^ cf)
            base = n * plan.used
            misc[r * cols + c, 0 : plan.folded, :] = ref[base + plan.nb : base + plan.used, :]
            v = jnp.where(live_row, ref[base : base + slot, :], 0.0)
            span = pl.ds(pl.multiple_of(c * slot, slot), slot)
            if per == 1:
                mat[r, span, :] = v
            else:
                mat[r // per, span, :] += pltpu.roll(v, (r % per) * plan.wide, 1)

    lane = lax.broadcasted_iota(I32, (plan.folded, LANES), 1) // plan.local

    def codes(first):
        got = [misc[first + e][0 : plan.folded] for e in range(plan.fold)]
        quads = []
        for g in range(plan.fold):
            quad = None
            for e in range(plan.fold):
                v = got[e]
                if e != g:
                    v = pltpu.roll(v, ((e - g) * plan.local) % LANES, 1)
                quad = v if quad is None else jnp.where(lane == e, v, quad)
            quads.append(quad)
        return jnp.concatenate(quads, axis=0).astype(I32)

    n_tile = depth // LANES
    jcode = codes(me_c * rows + chunk * plan.fold)
    icopy = pltpu.make_async_copy(ivec, idx, sem.at[0])
    jcopy = pltpu.make_async_copy(jvec, jdx, sem.at[1])

    @pl.when(me_r >= 0)
    def _():
        jvec[...] = codes(me_c * rows + chunk * plan.fold)[slots:] * n_tile
        jcopy.start()
        for t in range(tiles):
            ivec[t] = codes(me_r * cols + t * plan.fold) * slots
        icopy.start()

    depth_iota = lax.broadcasted_iota(I32, (depth, LANES), 0)
    ra = lax.broadcasted_iota(I32, (LANES, LANES), 0)
    rb = lax.broadcasted_iota(I32, (LANES, LANES), 1)

    def tile(i, j):
        return mat[j, i * LANES : (i + 1) * LANES, :]

    def put_x(i, j, v):
        hi = v.astype(BF16)
        lo = (v - hi.astype(F32)).astype(BF16)
        left[i * LANES : (i + 1) * LANES, j * LANES : (j + 1) * LANES] = hi
        left[depth + i * LANES : depth + (i + 1) * LANES, j * LANES : (j + 1) * LANES] = lo

    def put_z(i, j, v):
        zrow[pl.ds(8 + i * LANES * n_tile + j, LANES, stride=n_tile), :] = v

    for i in range(n_tile):
        for j in range(i, n_tile):
            v = tile(j, i)
            if i == j:
                diag = None
                for g in range(per):
                    spot = g * plan.wide + plan.nb
                    col = jnp.broadcast_to(v[:, spot : spot + 1], v.shape)
                    diag = col if diag is None else jnp.where(ra // plan.wide == g, col, diag)
                put_z(i, i, jnp.where(ra > rb, v, jnp.where(ra == rb, diag, v.T)))
            else:
                put_z(j, i, v)
                put_z(i, j, v.T)
    for l in range(slots):
        at = jcode[l : l + 1, :]
        pick[:, l * LANES : (l + 1) * LANES] = jnp.where(depth_iota == at, 1.0, 0.0).astype(BF16)
    for i in range(n_tile):
        for j in range(i, n_tile):
            v = tile(i, j)
            if i == j:
                put_x(i, i, jnp.where(ra <= rb, v, v.T))
            else:
                put_x(i, j, v)
                put_x(j, i, v.T)

    group = lax.broadcasted_iota(I32, (8, LANES), 0) // n_tile
    jcopy.wait()

    def gather_rows(l):
        for j in range(0, LANES, 8 // n_tile):
            both = None
            for e in range(8 // n_tile):
                at = pl.multiple_of(jdx[l, j + e], n_tile)
                v = zrow[pl.ds(at + (8 - e * n_tile), 8), :]
                both = v if both is None else jnp.where(group == e, v, both)
            base = (l * LANES + j) * n_tile
            zgot[base : base + 8, :] = both
        for s in range(n_tile):
            v = zgot[pl.ds(l * LANES * n_tile + s, LANES, stride=n_tile), :]
            zj[pl.ds(s * LANES * slots + l, LANES, stride=slots), :] = v.T

    for m in range(slots // 2):
        res = jnp.dot(left[...], pick[:, m * 256 : (m + 1) * 256], preferred_element_type=F32)
        res = res[:depth] + res[depth:]
        for l in range(2):
            xj[pl.ds(2 * m + l, depth, stride=slots), :] = res[:, l * LANES : (l + 1) * LANES]
    for l in range(slots):
        gather_rows(l)
    icopy.wait()

    def eight(tile_at, n):
        base = n * 8
        for s in range(8):
            total = None
            for k in range(slots):
                q = pl.multiple_of(idx[tile_at, slots + k, base + s], slots)
                p = pl.multiple_of(idx[tile_at, k, base + s], slots)
                term = xj[pl.ds(q, slots), :] * zj[pl.ds(p, slots), :]
                total = term if total is None else total + term
            acc[s * slots : (s + 1) * slots, :] = total
        out = None
        for l in range(slots):
            v = acc[pl.ds(l, 8, stride=slots), :]
            out = v if out is None else out + v
        out_ref[tile_at * LANES + base : tile_at * LANES + base + 8, :] = out

    outs = []
    for t in range(tiles):
        for n in range(LANES // 8):
            eight(t, n)
        span = pl.ds(t * LANES, LANES)
        there = out_hbm.at[span, pl.ds(pl.multiple_of(chunk * LANES, LANES), LANES)]
        outs.append(pltpu.make_async_copy(out_ref.at[span], there, osem.at[t]))
        outs[-1].start()
    for copy in outs:
        copy.wait()


def send(plan, v, row_xor, col_xor):
    size = plan.cols
    pairs = []
    for r, c in itertools.product(range(plan.rows), range(plan.cols)):
        pairs.append((r * size + c, (r ^ row_xor) * size + (c ^ col_xor)))
    return lax.ppermute(v, ("row", "col"), pairs)


def stack_kernel(plan, *refs):
    for n, ref in enumerate(refs[:-1]):
        refs[-1][n * plan.used : (n + 1) * plan.used, :] = ref[0 : plan.used, :]


def gather(plan, v):
    line = [v if k == (0, 0) else send(plan, v, *k) for k in plan.far]
    stack = pl.pallas_call(
        functools.partial(stack_kernel, plan),
        out_shape=jax.ShapeDtypeStruct((len(line) * plan.used, LANES), F32),
        compiler_params=pltpu.CompilerParams(vmem_limit_bytes=4 << 20),
        name="stack",
    )(*line)
    stacks = [stack if k == (0, 0) else send(plan, stack, *k) for k in plan.near]
    return stacks + [send(plan, s, 1, 0) for s in stacks]


def schur_call(plan, stacks):
    n_tile = plan.depth // LANES
    return pl.pallas_call(
        functools.partial(main_kernel, plan, len(stacks)),
        grid=(plan.nj // LANES,),
        in_specs=[pl.BlockSpec(memory_space=pltpu.VMEM)] * len(stacks),
        out_specs=pl.BlockSpec(memory_space=pltpu.HBM),
        out_shape=jax.ShapeDtypeStruct((plan.ni, plan.nj), F32),
        scratch_shapes=[
            pltpu.VMEM((plan.ni, LANES), F32),
            pltpu.SemaphoreType.DMA((plan.ni // LANES,)),
            pltpu.VMEM((plan.rows * plan.cols, EXTRA, LANES), F32),
            pltpu.VMEM((n_tile, plan.depth, LANES), F32),
            pltpu.VMEM((2 * plan.depth, plan.depth), BF16),
            pltpu.VMEM((plan.depth * n_tile + 16, LANES), F32),
            pltpu.VMEM((plan.slots * LANES * n_tile, LANES), F32),
            pltpu.VMEM((plan.depth * plan.slots, LANES), F32),
            pltpu.VMEM((plan.depth * plan.slots, LANES), F32),
            pltpu.VMEM((plan.depth, plan.slots * LANES), BF16),
            pltpu.VMEM((plan.ni // LANES, 2 * plan.slots, LANES), I32),
            pltpu.VMEM((plan.slots, LANES), I32),
            pltpu.VMEM((8 * plan.slots, LANES), F32),
            pltpu.SMEM((plan.ni // LANES, 2 * plan.slots, LANES), I32),
            pltpu.SMEM((plan.slots, LANES), I32),
            pltpu.SemaphoreType.DMA((2,)),
        ],
        compiler_params=pltpu.CompilerParams(vmem_limit_bytes=24 << 20),
        name="schur",
    )(*stacks)


def shards(rows, cols, moment_x, zinv, positions, entry_count):
    plan = Plan(rows, cols, moment_x.shape, positions.shape)
    args = (moment_x.T, zinv.T, positions.T, entry_count.reshape(1, -1))
    packed = pl.pallas_call(
        functools.partial(pack_kernel, plan),
        in_specs=[pl.BlockSpec(memory_space=pltpu.HBM)] * 4,
        out_shape=jax.ShapeDtypeStruct((plan.payload, LANES), F32),
        scratch_shapes=[
            pltpu.VMEM((plan.nb, plan.mb), F32),
            pltpu.VMEM((plan.nb, plan.mb), F32),
            pltpu.VMEM((2 * plan.slots, plan.local), I32),
            pltpu.VMEM((1, plan.local), I32),
            pltpu.SemaphoreType.DMA((4,)),
        ],
        compiler_params=pltpu.CompilerParams(vmem_limit_bytes=4 << 20),
        name="pack",
    )(*[pltpu.with_memory_space_constraint(v, pltpu.HBM) for v in args])
    return schur_call(plan, gather(plan, packed))


def solution(mesh):
    return jax.shard_map(
        functools.partial(shards, mesh.shape["row"], mesh.shape["col"]),
        mesh=mesh,
        in_specs=(P("row", "col"), P("row", "col"), P(("row", "col"), None), P(("row", "col"))),
        out_specs=P("row", "col"),
        check_vma=False,
    )
```

```python
import functools
import itertools
import jax
import jax.numpy as jnp
from jax import lax
from jax.experimental import pallas as pl
from jax.experimental.pallas import tpu as pltpu
from jax.sharding import PartitionSpec as P

LANES = 128
F32, BF16, I32 = jnp.float32, jnp.bfloat16, jnp.int32
EXTRA = 8


class Plan:
    def __init__(self, rows, cols, x_shape, pos_shape):
        self.rows, self.cols = rows, cols
        self.mb, self.nb = x_shape
        self.halves = self.mb // self.nb
        self.slot = 1 << self.nb.bit_length()
        self.wide = self.halves * self.slot
        self.depth = cols * self.slot
        self.dead = self.slot - 1
        self.local, self.slots = pos_shape[0], pos_shape[1] // 2
        self.fold = LANES // self.local
        self.folded = 2 * self.slots // self.fold
        self.ni = self.local * cols
        self.nj = self.local * rows
        self.used = self.nb + self.folded
        self.payload = -(-max(self.slot, self.used) // 8) * 8
        row_bits, col_bits = rows.bit_length() - 1, cols.bit_length() - 1
        y_bits = col_bits // 2
        self.far = [(0, k << y_bits) for k in range(1 << (col_bits - y_bits))]
        self.near = [(i << 1, k) for i in range(1 << (row_bits - 1)) for k in range(1 << y_bits)]


def pack_kernel(plan, x_in, z_in, pos_in, cnt_in, out_ref, x_ref, z_ref, pos_ref, cnt_ref, sem):
    nb, slot, wide = plan.nb, plan.slot, plan.wide
    me_r, me_c = lax.axis_index("row"), lax.axis_index("col")
    copies = []
    for n, (src, dst) in enumerate(((x_in, x_ref), (z_in, z_ref), (pos_in, pos_ref), (cnt_in, cnt_ref))):
        copies.append(pltpu.make_async_copy(src, dst, sem.at[n]))
        copies[-1].start()
    out_ref[...] = jnp.zeros_like(out_ref)
    for copy in copies:
        copy.wait()
    a = lax.broadcasted_iota(I32, (nb, plan.mb), 0) + me_c * nb
    b = lax.broadcasted_iota(I32, (nb, plan.mb), 1) + me_r * plan.mb
    z = z_ref[...]
    mixed = jnp.where(a <= b, x_ref[...], z)
    diag = jnp.sum(jnp.where(a == b, z, 0.0), axis=1, keepdims=True)
    for h in range(plan.halves):
        out_ref[0:nb, h * slot : h * slot + nb] = mixed[:, h * nb : (h + 1) * nb]
    out_ref[0:nb, nb : nb + 1] = diag
    spots = pos_ref[...].astype(F32)
    code = spots
    for t in range(1, plan.cols):
        code = code + jnp.where(spots >= float(t * nb), float(slot - nb), 0.0)
    k = lax.broadcasted_iota(I32, code.shape, 0) % plan.slots
    code = jnp.where(k < cnt_ref[...], code, float(plan.dead))
    for g in range(plan.fold):
        piece = code[g * plan.folded : (g + 1) * plan.folded, :]
        out_ref[nb : nb + plan.folded, g * plan.local : (g + 1) * plan.local] = piece


def place(plan, near, ins, misc, mat):
    slot, cols = plan.slot, plan.cols
    me_r, me_c = lax.axis_index("row"), lax.axis_index("col")
    per = LANES // plan.wide
    live_row = lax.broadcasted_iota(I32, (slot, LANES), 0) < plan.nb
    for ref, (ri, ci) in zip(ins, near):
        for n, (rf, cf) in enumerate(plan.far):
            r, c = me_r ^ (ri ^ rf), me_c ^ (ci ^ cf)
            base = n * plan.used
            misc[r * cols + c, 0 : plan.folded, :] = ref[base + plan.nb : base + plan.used, :]
            v = jnp.where(live_row, ref[base : base + slot, :], 0.0)
            span = pl.ds(pl.multiple_of(c * slot, slot), slot)
            if per == 1:
                mat[r, span, :] = v
            else:
                mat[r // per, span, :] += pltpu.roll(v, (r % per) * plan.wide, 1)


def early_kernel(plan, near, *refs):
    misc, mat = refs[-2:]
    if LANES // plan.wide > 1:
        mat[...] = jnp.zeros_like(mat)
    place(plan, near, refs[:-2], misc, mat)


def main_kernel(plan, near, *refs):
    n_in = len(near)
    ins, (out_hbm, misc, mat) = refs[:n_in], refs[n_in + 2 : n_in + 5]
    out_ref, osem, left, zrow, zgot, xj, zj, pick, ivec, jvec, acc, idx, jdx, sem = refs[n_in + 5 :]
    slot, cols, rows = plan.slot, plan.cols, plan.rows
    slots, tiles, depth = plan.slots, plan.ni // LANES, plan.depth
    me_r, me_c = lax.axis_index("row"), lax.axis_index("col")
    chunk = pl.program_id(0)
    per = LANES // plan.wide

    @pl.when(chunk == 0)
    def _():
        place(plan, near, ins, misc, mat)

    lane = lax.broadcasted_iota(I32, (plan.folded, LANES), 1) // plan.local

    def codes(first):
        got = [misc[first + e][0 : plan.folded] for e in range(plan.fold)]
        quads = []
        for g in range(plan.fold):
            quad = None
            for e in range(plan.fold):
                v = got[e]
                if e != g:
                    v = pltpu.roll(v, ((e - g) * plan.local) % LANES, 1)
                quad = v if quad is None else jnp.where(lane == e, v, quad)
            quads.append(quad)
        return jnp.concatenate(quads, axis=0).astype(I32)

    n_tile = depth // LANES
    jcode = codes(me_c * rows + chunk * plan.fold)
    icopy = pltpu.make_async_copy(ivec, idx, sem.at[0])
    jcopy = pltpu.make_async_copy(jvec, jdx, sem.at[1])

    @pl.when(me_r >= 0)
    def _():
        jvec[...] = codes(me_c * rows + chunk * plan.fold)[slots:] * n_tile
        jcopy.start()
        for t in range(tiles):
            ivec[t] = codes(me_r * cols + t * plan.fold) * slots
        icopy.start()

    depth_iota = lax.broadcasted_iota(I32, (depth, LANES), 0)
    ra = lax.broadcasted_iota(I32, (LANES, LANES), 0)
    rb = lax.broadcasted_iota(I32, (LANES, LANES), 1)

    def tile(i, j):
        return mat[j, i * LANES : (i + 1) * LANES, :]

    def put_x(i, j, v):
        hi = v.astype(BF16)
        lo = (v - hi.astype(F32)).astype(BF16)
        left[i * LANES : (i + 1) * LANES, j * LANES : (j + 1) * LANES] = hi
        left[depth + i * LANES : depth + (i + 1) * LANES, j * LANES : (j + 1) * LANES] = lo

    def put_z(i, j, v):
        zrow[pl.ds(8 + i * LANES * n_tile + j, LANES, stride=n_tile), :] = v

    for i in range(n_tile):
        for j in range(i, n_tile):
            v = tile(j, i)
            if i == j:
                diag = None
                for g in range(per):
                    spot = g * plan.wide + plan.nb
                    col = jnp.broadcast_to(v[:, spot : spot + 1], v.shape)
                    diag = col if diag is None else jnp.where(ra // plan.wide == g, col, diag)
                put_z(i, i, jnp.where(ra > rb, v, jnp.where(ra == rb, diag, v.T)))
            else:
                put_z(j, i, v)
                put_z(i, j, v.T)
    for l in range(slots):
        at = jcode[l : l + 1, :]
        pick[:, l * LANES : (l + 1) * LANES] = jnp.where(depth_iota == at, 1.0, 0.0).astype(BF16)
    for i in range(n_tile):
        for j in range(i, n_tile):
            v = tile(i, j)
            if i == j:
                put_x(i, i, jnp.where(ra <= rb, v, v.T))
            else:
                put_x(i, j, v)
                put_x(j, i, v.T)

    group = lax.broadcasted_iota(I32, (8, LANES), 0) // n_tile
    jcopy.wait()

    def gather_rows(l):
        for j in range(0, LANES, 8 // n_tile):
            both = None
            for e in range(8 // n_tile):
                at = pl.multiple_of(jdx[l, j + e], n_tile)
                v = zrow[pl.ds(at + (8 - e * n_tile), 8), :]
                both = v if both is None else jnp.where(group == e, v, both)
            base = (l * LANES + j) * n_tile
            zgot[base : base + 8, :] = both

    def turn(l):
        for s in range(n_tile):
            v = zgot[pl.ds(l * LANES * n_tile + s, LANES, stride=n_tile), :]
            zj[pl.ds(s * LANES * slots + l, LANES, stride=slots), :] = v.T

    for m in range(slots // 2):
        res = jnp.dot(left[...], pick[:, m * 256 : (m + 1) * 256], preferred_element_type=F32)
        res = res[:depth] + res[depth:]
        for l in range(2):
            xj[pl.ds(2 * m + l, depth, stride=slots), :] = res[:, l * LANES : (l + 1) * LANES]
    gather_rows(0)
    for l in range(slots):
        if l + 1 < slots:
            gather_rows(l + 1)
        turn(l)
    icopy.wait()

    def eight(tile_at, n):
        base = n * 8
        for s in range(8):
            total = None
            for k in range(slots):
                q = pl.multiple_of(idx[tile_at, slots + k, base + s], slots)
                p = pl.multiple_of(idx[tile_at, k, base + s], slots)
                term = xj[pl.ds(q, slots), :] * zj[pl.ds(p, slots), :]
                total = term if total is None else total + term
            acc[s * slots : (s + 1) * slots, :] = total
        out = None
        for l in range(slots):
            v = acc[pl.ds(l, 8, stride=slots), :]
            out = v if out is None else out + v
        out_ref[tile_at * LANES + base : tile_at * LANES + base + 8, :] = out

    outs = []
    for t in range(tiles):
        for n in range(LANES // 8):
            eight(t, n)
        span = pl.ds(t * LANES, LANES)
        there = out_hbm.at[span, pl.ds(pl.multiple_of(chunk * LANES, LANES), LANES)]
        outs.append(pltpu.make_async_copy(out_ref.at[span], there, osem.at[t]))
        outs[-1].start()
    for copy in outs:
        copy.wait()


def send(plan, v, row_xor, col_xor):
    size = plan.cols
    pairs = []
    for r, c in itertools.product(range(plan.rows), range(plan.cols)):
        pairs.append((r * size + c, (r ^ row_xor) * size + (c ^ col_xor)))
    return lax.ppermute(v, ("row", "col"), pairs)


def stack_kernel(plan, *refs):
    for n, ref in enumerate(refs[:-1]):
        refs[-1][n * plan.used : (n + 1) * plan.used, :] = ref[0 : plan.used, :]


def gather(plan, v):
    line = [v if k == (0, 0) else send(plan, v, *k) for k in plan.far]
    stack = pl.pallas_call(
        functools.partial(stack_kernel, plan),
        out_shape=jax.ShapeDtypeStruct((len(line) * plan.used, LANES), F32),
        compiler_params=pltpu.CompilerParams(vmem_limit_bytes=4 << 20),
        name="stack",
    )(*line)
    stacks = [stack if k == (0, 0) else send(plan, stack, *k) for k in plan.near]
    return stacks + [send(plan, s, 1, 0) for s in stacks]


def schur_call(plan, stacks):
    n_tile = plan.depth // LANES
    vmem = pl.BlockSpec(memory_space=pltpu.VMEM)
    near = [(core ^ i, k) for core in (0, 1) for i, k in plan.near]
    first = len(plan.near) + 1
    held = (
        jax.ShapeDtypeStruct((plan.rows * plan.cols, EXTRA, LANES), F32),
        jax.ShapeDtypeStruct((n_tile, plan.depth, LANES), F32),
    )
    misc, mat = pl.pallas_call(
        functools.partial(early_kernel, plan, near[:first]),
        in_specs=[vmem] * first,
        out_specs=(vmem, vmem),
        out_shape=held,
        cost_estimate=pl.CostEstimate(flops=1 << 22, bytes_accessed=1 << 20, transcendentals=0),
        compiler_params=pltpu.CompilerParams(vmem_limit_bytes=8 << 20),
        name="early",
    )(*stacks[:first])
    late = near[first:]
    return pl.pallas_call(
        functools.partial(main_kernel, plan, late),
        grid=(plan.nj // LANES,),
        in_specs=[vmem] * (len(late) + 2),
        out_specs=(pl.BlockSpec(memory_space=pltpu.HBM), vmem, vmem),
        out_shape=(jax.ShapeDtypeStruct((plan.ni, plan.nj), F32), *held),
        input_output_aliases={len(late): 1, len(late) + 1: 2},
        scratch_shapes=[
            pltpu.VMEM((plan.ni, LANES), F32),
            pltpu.SemaphoreType.DMA((plan.ni // LANES,)),
            pltpu.VMEM((2 * plan.depth, plan.depth), BF16),
            pltpu.VMEM((plan.depth * n_tile + 16, LANES), F32),
            pltpu.VMEM((plan.slots * LANES * n_tile, LANES), F32),
            pltpu.VMEM((plan.depth * plan.slots, LANES), F32),
            pltpu.VMEM((plan.depth * plan.slots, LANES), F32),
            pltpu.VMEM((plan.depth, plan.slots * LANES), BF16),
            pltpu.VMEM((plan.ni // LANES, 2 * plan.slots, LANES), I32),
            pltpu.VMEM((plan.slots, LANES), I32),
            pltpu.VMEM((8 * plan.slots, LANES), F32),
            pltpu.SMEM((plan.ni // LANES, 2 * plan.slots, LANES), I32),
            pltpu.SMEM((plan.slots, LANES), I32),
            pltpu.SemaphoreType.DMA((2,)),
        ],
        compiler_params=pltpu.CompilerParams(vmem_limit_bytes=24 << 20),
        name="schur",
    )(*stacks[first:], misc, mat)[0]


def shards(rows, cols, moment_x, zinv, positions, entry_count):
    plan = Plan(rows, cols, moment_x.shape, positions.shape)
    args = (moment_x.T, zinv.T, positions.T, entry_count.reshape(1, -1))
    packed = pl.pallas_call(
        functools.partial(pack_kernel, plan),
        in_specs=[pl.BlockSpec(memory_space=pltpu.HBM)] * 4,
        out_shape=jax.ShapeDtypeStruct((plan.payload, LANES), F32),
        scratch_shapes=[
            pltpu.VMEM((plan.nb, plan.mb), F32),
            pltpu.VMEM((plan.nb, plan.mb), F32),
            pltpu.VMEM((2 * plan.slots, plan.local), I32),
            pltpu.VMEM((1, plan.local), I32),
            pltpu.SemaphoreType.DMA((4,)),
        ],
        compiler_params=pltpu.CompilerParams(vmem_limit_bytes=4 << 20),
        name="pack",
    )(*[pltpu.with_memory_space_constraint(v, pltpu.HBM) for v in args])
    return schur_call(plan, gather(plan, packed))


def solution(mesh):
    return jax.shard_map(
        functools.partial(shards, mesh.shape["row"], mesh.shape["col"]),
        mesh=mesh,
        in_specs=(P("row", "col"), P("row", "col"), P(("row", "col"), None), P(("row", "col"))),
        out_specs=P("row", "col"),
        check_vma=False,
    )
```
